128 devices in a mesh: rows: 64 (over y, x, z), grp: 2 (over core).
Axes of the slice: x: 4, y: 4, z: 4, core: 2. Of those that a mesh axis runs over, the one named last changes fastest.
Arguments:
- snap_early: float32 [12288, 128, 128], P(('rows', 'grp')), as said below
- snap_late: float32 [12288, 128, 128], P(('rows', 'grp')), as said below
- block_ids: int32 [12288], P(('rows', 'grp')), may hold values from 0 to 12287, as said below
- block_owner: int32 [12288], replicated, may hold values from 0 to 127, as said below
- block_slot: int32 [12288], replicated, may hold values from 0 to 127, as said below
Outputs:
- modes: float32 [16384, 128, 128], P(('rows', 'grp'))
- operator: float32 [128, 128], replicated
The draws below stay inside these ranges and needn't reach their ends.
Inputs may be any that keep to these rules, and one draw needn't show every extreme that they name: block_ids is a permutation of 0 to 12287. `block_owner`: each analysis device owns at most 128 blocks and one owns exactly 128; among the blocks of one solver device (aligned runs of 96 slots of block_ids) at most 1 go to one analysis device, and in every draw some solver device sends exactly 1 to one. `block_slot`: the blocks of one analysis device take the slots 0 to c - 1, each once, where c is their count. `snap_early`: Real-valued snapshots with magnitudes from below one to some thousands, row and column scales spread by up to a factor of about 900; the matrix of all rows has full column rank. `snap_late`: Real-valued snapshots, the early ones advanced by one step of a linear flow plus noise.
All inputs are finite; a program needn't handle non-finite values.
Results may differ from the reference program's by a relative error of at most 0.0003.
Values sent between devices are 32-bit elements; how exact they have to be, the bound alone decides.
No kernel may reach another device: no remote copies, remote signals or barrier semaphores. Data moves between devices by JAX's collectives and lax.ppermute only.
A program may use at most 128 MiB of HBM per device.

```python
import math
import jax
import jax.numpy as jnp
from jax import lax

K = 128
BLOCK = 128
SB_DEV = 96
CAP = 128
NBLOCKS = 12288
SLOTS_ALL = 16384


def snapshot_pair(key):
    keys = jax.random.split(jax.random.fold_in(key, 7), 7)
    row_total = NBLOCKS * BLOCK
    members = NBLOCKS // SB_DEV
    spread = math.log(10.0)
    normal_part = jax.random.normal(keys[0], (row_total, K), jnp.float32)
    mixing = jnp.eye(K, dtype=jnp.float32) + 0.3 * jax.random.normal(keys[1], (K, K), jnp.float32) / math.sqrt(K)
    column_scale = jnp.exp(jax.random.uniform(keys[2], (K,), jnp.float32, 0.0, math.log(10.0)))
    device_rank = (jnp.arange(row_total) // (SB_DEV * BLOCK)).astype(jnp.float32)
    ramp = 1.0 + 2.0 * device_rank / max(members - 1, 1)
    row_scale = jnp.exp(jax.random.uniform(keys[3], (row_total,), jnp.float32, 0.0, spread)) * ramp
    early_rows = row_scale[:, None] * jnp.dot(normal_part, mixing, precision=lax.Precision.HIGHEST) * column_scale[None, :]
    dynamics = 0.8 * jnp.eye(K, dtype=jnp.float32) + 0.5 * jax.random.normal(keys[5], (K, K), jnp.float32) / math.sqrt(K)
    noise = jax.random.normal(keys[6], (row_total, K), jnp.float32) * (0.3 * row_scale)[:, None] * column_scale[None, :]
    late_rows = jnp.dot(early_rows, dynamics, precision=lax.Precision.HIGHEST) + noise
    return (early_rows.reshape((NBLOCKS, BLOCK, K)), late_rows.reshape((NBLOCKS, BLOCK, K)))


def block_routing(key):
    keys = jax.random.split(jax.random.fold_in(key, 11), 3)
    members = NBLOCKS // SB_DEV
    spread = CAP - SB_DEV
    halves = members // 2
    order = jax.random.permutation(keys[0], members).astype(jnp.int32)
    deltas = jax.random.randint(keys[1], (halves,), 0, spread + 1).astype(jnp.int32).at[0].set(spread)
    counts = jnp.full((members,), SB_DEV, jnp.int32)
    counts = counts.at[order[:halves]].add(deltas).at[order[halves:2 * halves]].add(-deltas)
    ends = jnp.cumsum(counts).astype(jnp.int32)
    position = jnp.arange(NBLOCKS, dtype=jnp.int32)
    owner_at = jnp.sum((position[:, None] >= ends[None, :]).astype(jnp.int32), axis=1).astype(jnp.int32)
    starts = ends - counts
    slot_at = (position - starts[owner_at]).astype(jnp.int32)
    solver_slot = (position % members * SB_DEV + position // members).astype(jnp.int32)
    labels = jax.random.permutation(keys[2], NBLOCKS).astype(jnp.int32)
    identity_map = jnp.zeros((NBLOCKS,), jnp.int32).at[solver_slot].set(labels)
    owners = jnp.zeros((NBLOCKS,), jnp.int32).at[labels].set(owner_at)
    slots = jnp.zeros((NBLOCKS,), jnp.int32).at[labels].set(slot_at)
    return (identity_map, owners, slots)


def draw_snap_early(key, part):
    return snapshot_pair(key)[0]


def draw_snap_late(key, part):
    return snapshot_pair(key)[1]


def draw_block_ids(key, part):
    return block_routing(key)[0]


def draw_block_owner(key, part):
    return block_routing(key)[1]


def draw_block_slot(key, part):
    return block_routing(key)[2]


def setup_inputs(seed: int = 0) -> dict:
    streams_of = jax.random.split(jax.random.key(seed), 6)
    return {
        "snap_early": draw_snap_early(jax.random.fold_in(streams_of[5], 71), 0),
        "snap_late": draw_snap_late(jax.random.fold_in(streams_of[5], 71), 0),
        "block_ids": draw_block_ids(jax.random.fold_in(streams_of[5], 71), 0),
        "block_owner": draw_block_owner(jax.random.fold_in(streams_of[5], 71), 0),
        "block_slot": draw_block_slot(jax.random.fold_in(streams_of[5], 71), 0),
    }


def upper_factor(gram_total):
    order = gram_total.shape[0]
    index = jnp.arange(order, dtype=jnp.int32)

    def step(j, factor):
        column = lax.dynamic_slice_in_dim(factor, j, 1, 1)[:, 0]
        grow = lax.dynamic_slice_in_dim(gram_total, j, 1, 0)[0]
        rest = grow - jnp.dot(column, factor, precision=lax.Precision.HIGHEST)
        pivot = jnp.sqrt(jnp.sum(jnp.where(index == j, rest, 0.0)))
        newrow = jnp.where(index >= j, rest / pivot, 0.0)
        picked = (index == j).astype(gram_total.dtype)
        return factor + picked[:, None] * newrow[None, :]
    return lax.fori_loop(0, order, step, jnp.zeros_like(gram_total))

def upper_inverse(factor):
    order = factor.shape[0]
    index = jnp.arange(order, dtype=jnp.int32)

    def step(t, inverse):
        i = order - 1 - t
        frow = lax.dynamic_slice_in_dim(factor, i, 1, 0)[0]
        unit = (index == i).astype(factor.dtype)
        diagonal = jnp.sum(frow * unit)
        newrow = (unit - jnp.dot(frow, inverse, precision=lax.Precision.HIGHEST)) / diagonal
        return inverse + unit[:, None] * newrow[None, :]
    return lax.fori_loop(0, order, step, jnp.zeros_like(factor))

def reference(snap_early, snap_late, block_ids, block_owner, block_slot):
    row_total = snap_early.shape[0] * snap_early.shape[1]
    early_rows = snap_early.reshape((row_total, snap_early.shape[2]))
    late_rows = snap_late.reshape((row_total, snap_late.shape[2]))
    gram_total = jnp.einsum('rk,rl->kl', early_rows, early_rows, precision=lax.Precision.HIGHEST) / row_total
    cross_total = jnp.einsum('rk,rl->kl', early_rows, late_rows, precision=lax.Precision.HIGHEST) / row_total
    factor = upper_factor(gram_total)
    inverse = upper_inverse(factor)
    coupled = jnp.dot(cross_total, inverse, precision=lax.Precision.HIGHEST)
    operator = jnp.dot(inverse.T, coupled, precision=lax.Precision.HIGHEST)
    solved = jnp.dot(late_rows, inverse, precision=lax.Precision.HIGHEST)
    mode_blocks = solved.reshape(snap_late.shape)
    position = (block_owner[block_ids] * CAP + block_slot[block_ids]).astype(jnp.int32)
    output = jnp.zeros((SLOTS_ALL, snap_late.shape[1], snap_late.shape[2]), mode_blocks.dtype)
    output = output.at[position].set(mode_blocks)
    return (output, operator)
```

```python
import functools

import jax
import jax.numpy as jnp
from jax import lax
from jax.experimental import pallas as pl
from jax.experimental.pallas import tpu as pltpu
from jax.sharding import PartitionSpec as P

AXES = ("rows", "grp")
CHUNKS = 2
GRAM_STEP = 8
ROWS = 8
APPLY_STEP = 16


def split_pair(x):
    hi = x.astype(jnp.bfloat16)
    lo = (x - hi.astype(jnp.float32)).astype(jnp.bfloat16)
    return hi, lo


def contract_rows(a, b):
    return lax.dot_general(
        a, b, (((0,), (0,)), ((), ())), preferred_element_type=jnp.float32
    )


def pack_kernel(height, lo, dest_ref, late_ref, out_ref, buf, sem_in, sem_out):
    count = late_ref.shape[0]

    def load(i):
        return pltpu.make_async_copy(
            late_ref.at[i, pl.ds(lo, height)], buf.at[dest_ref[i]], sem_in
        )

    def start(i, carry):
        load(i).start()
        return carry

    lax.fori_loop(0, count, start, 0)
    pltpu.make_async_copy(
        late_ref.at[pl.ds(0, count), pl.ds(lo, height)], buf.at[pl.ds(0, count)], sem_in
    ).wait()
    out = pltpu.make_async_copy(buf, out_ref, sem_out)
    out.start()
    out.wait()


def pack(late, dest, members, lo, height):
    width = late.shape[2]
    return pl.pallas_call(
        functools.partial(pack_kernel, height, lo),
        grid_spec=pltpu.PrefetchScalarGridSpec(
            num_scalar_prefetch=1,
            grid=(1,),
            in_specs=[pl.BlockSpec(memory_space=pl.ANY)],
            out_specs=pl.BlockSpec(memory_space=pl.ANY),
            scratch_shapes=[
                pltpu.VMEM((members, height, width), jnp.float32),
                pltpu.SemaphoreType.DMA,
                pltpu.SemaphoreType.DMA,
            ],
        ),
        out_shape=jax.ShapeDtypeStruct((members, height, width), jnp.float32),
        cost_estimate=pl.CostEstimate(flops=100000000, bytes_accessed=1 << 23, transcendentals=0),
        name="pack",
    )(dest, late)


def gram_kernel(note_ref, early_ref, late_ref, out_ref, acc):
    step = pl.program_id(0)

    @pl.when(step == 0)
    def _():
        acc[...] = jnp.zeros_like(acc)

    width = early_ref.shape[2]
    early = early_ref[...].reshape((-1, width))
    late = late_ref[...].reshape((-1, width))
    ehi, elo = split_pair(early)
    lhi, llo = split_pair(late)
    acc[...] += contract_rows(
        jnp.concatenate([ehi, lhi, llo], axis=1), jnp.concatenate([ehi, elo], axis=1)
    )

    @pl.when(step == pl.num_programs(0) - 1)
    def _():
        mixed = acc[0:width, width:]
        gram = acc[0:width, 0:width] + (mixed + mixed.T)
        flipped = (
            acc[width : 2 * width, 0:width]
            + acc[width : 2 * width, width:]
            + acc[2 * width :, 0:width]
        )
        out_ref[...] = jnp.zeros_like(out_ref)
        out_ref[:, 0, :] = gram
        out_ref[:, 1, :] = flipped.T
        out_ref[:, 2, :] = note_ref[...]


def gram_pair(note, early, late):
    count, block, width = early.shape
    spec = pl.BlockSpec((GRAM_STEP, block, width), lambda i: (i, 0, 0))
    flops = 2 * count * block * 6 * width * width
    return pl.pallas_call(
        gram_kernel,
        grid=(count // GRAM_STEP,),
        in_specs=[pl.BlockSpec(note.shape, lambda i: (0, 0)), spec, spec],
        out_specs=pl.BlockSpec((width, ROWS, width), lambda i: (0, 0, 0)),
        out_shape=jax.ShapeDtypeStruct((width, ROWS, width), jnp.float32),
        scratch_shapes=[pltpu.VMEM((3 * width, 2 * width), jnp.float32)],
        cost_estimate=pl.CostEstimate(flops=flops, bytes_accessed=1 << 23, transcendentals=0),
        name="gram",
    )(note, early, late)


def dot3(a, b):
    return jnp.dot(a, b, precision=lax.Precision.HIGHEST, preferred_element_type=jnp.float32)


def finish_kernel(row_total, stats_ref, weight_ref, operator_ref, work):
    order = stats_ref.shape[0]
    row_id = lax.broadcasted_iota(jnp.int32, (order, 1), 0)
    lane = lax.broadcasted_iota(jnp.int32, (1, 2 * order), 1)
    lane_half = lax.broadcasted_iota(jnp.int32, (1, order), 1)
    work[:, 0:order] = stats_ref[:, 0, :] / row_total
    work[:, order:] = (row_id == lane_half).astype(jnp.float32)

    def step(j, carry):
        row = work[pl.ds(j, 1), :]
        inv = lax.rsqrt(jnp.sum(jnp.where(lane == j, row, 0.0), axis=1, keepdims=True))
        scaled = row * inv
        table = work[...]
        column = jnp.sum(
            jnp.where(lane_half == j, table[:, 0:order], 0.0), axis=1, keepdims=True
        )
        down = jnp.where(row_id > j, column * inv, 0.0)
        work[...] = jnp.where(row_id == j, scaled, table - down * scaled)
        return carry

    lax.fori_loop(0, order, step, 0)
    inverse_t = work[:, order:]
    inverse = inverse_t.T
    cross = stats_ref[:, 1, :] / row_total
    operator_ref[...] = dot3(inverse_t, dot3(cross, inverse))
    whi, wlo = split_pair(inverse)
    weight_ref[0:order, 0:order] = whi
    weight_ref[0:order, order:] = wlo
    weight_ref[order:, 0:order] = whi
    weight_ref[order:, order:] = wlo


def finish(stats, row_total):
    order = stats.shape[0]
    return pl.pallas_call(
        functools.partial(finish_kernel, float(row_total)),
        out_shape=(
            jax.ShapeDtypeStruct((2 * order, 2 * order), jnp.bfloat16),
            jax.ShapeDtypeStruct((order, order), jnp.float32),
        ),
        scratch_shapes=[pltpu.VMEM((order, 2 * order), jnp.float32)],
        cost_estimate=pl.CostEstimate(flops=1000000000, bytes_accessed=1 << 19, transcendentals=0),
        name="finish",
    )(stats)


def apply_kernel(lo, place_ref, weight_ref, arrived_ref, *rest):
    out_ref, buf_in, buf_out, sem_in, sem_out = rest[-5:]
    count, height, width = arrived_ref.shape
    steps = count // APPLY_STEP

    def fetch(t, k):
        return pltpu.make_async_copy(
            arrived_ref.at[pl.ds(t * APPLY_STEP, APPLY_STEP)], buf_in.at[k], sem_in.at[k]
        )

    def drain(k):
        pltpu.make_async_copy(
            buf_out.at[k], out_ref.at[pl.ds(0, APPLY_STEP), pl.ds(lo, height)], sem_out.at[k]
        ).wait()

    fetch(0, 0).start()

    def step(t, carry):
        k = lax.rem(t, 2)

        @pl.when(t + 1 < steps)
        def _():
            fetch(t + 1, 1 - k).start()

        fetch(t, k).wait()

        @pl.when(t >= 2)
        def _():
            drain(k)

        rows = buf_in[k].reshape((APPLY_STEP * height, width))
        hi, lo_part = split_pair(rows)
        wide = jnp.dot(
            jnp.concatenate([hi, lo_part], axis=1),
            weight_ref[...],
            preferred_element_type=jnp.float32,
        )
        solved = wide[:, 0:width] + wide[:, width:]
        buf_out[k] = solved.reshape((APPLY_STEP, height, width))
        for i in range(APPLY_STEP):
            code = place_ref[t * APPLY_STEP + i]
            slot = jnp.bitwise_and(code, 127)

            @pl.when(code >= 128)
            def _():
                buf_out[k, i] = jnp.zeros((height, width), jnp.float32)

            pltpu.make_async_copy(
                buf_out.at[k, i], out_ref.at[slot, pl.ds(lo, height)], sem_out.at[k]
            ).start()
        return carry

    lax.fori_loop(0, steps, step, 0)
    drain(0)
    drain(1)


def apply_inverse(place, weight, arrived, modes, lo, block):
    count, height, width = arrived.shape
    whole = pl.BlockSpec(memory_space=pltpu.VMEM)
    anywhere = pl.BlockSpec(memory_space=pl.ANY)
    args = (place, weight, arrived) + (() if modes is None else (modes,))
    return pl.pallas_call(
        functools.partial(apply_kernel, lo),
        grid_spec=pltpu.PrefetchScalarGridSpec(
            num_scalar_prefetch=1,
            grid=(1,),
            in_specs=[whole, anywhere] + ([] if modes is None else [anywhere]),
            out_specs=anywhere,
            scratch_shapes=[
                pltpu.VMEM((2, APPLY_STEP, height, width), jnp.float32),
                pltpu.VMEM((2, APPLY_STEP, height, width), jnp.float32),
                pltpu.SemaphoreType.DMA((2,)),
                pltpu.SemaphoreType.DMA((2,)),
            ],
        ),
        out_shape=jax.ShapeDtypeStruct((count, block, width), jnp.float32),
        input_output_aliases={} if modes is None else {3: 0},
        cost_estimate=pl.CostEstimate(
            flops=8 * count * height * width * width, bytes_accessed=1 << 23, transcendentals=0
        ),
        name="apply",
    )(*args)


def exchange(payload):
    return lax.all_to_all(payload, AXES, split_axis=0, concat_axis=0, tiled=True)


def body(snap_early, snap_late, block_ids, block_owner, block_slot):
    members = lax.axis_size(AXES)
    count, block, width = snap_late.shape
    row_total = count * block * members
    labels = jnp.arange(block_owner.shape[0], dtype=jnp.int32)
    code = block_owner * 128 + block_slot
    hits = block_ids[:, None] == labels[None, :]
    code_here = jnp.sum(jnp.where(hits, code[None, :], 0), axis=1)
    dest = code_here // 128
    slot_here = code_here % 128
    height = block // CHUNKS
    sent = [
        exchange(pack(snap_late, dest, members, c * height, height)) for c in range(CHUNKS)
    ]
    target = jnp.arange(members, dtype=jnp.int32)
    note = jnp.sum(
        jnp.where(dest[None, :] == target[:, None], slot_here[None, :] + 1, 0), axis=1
    )
    note = jnp.broadcast_to(note.astype(jnp.float32)[:, None], (members, width))
    partial = exchange(gram_pair(note, snap_early, snap_late))
    mine = jnp.sum(partial, axis=0)
    stats = exchange(jnp.broadcast_to(mine[None], (members, ROWS, width)))
    weight, operator = finish(stats, row_total)
    slot_in = partial[:, 2, 0].astype(jnp.int32)
    empty = slot_in == 0
    filled = jnp.sum((slot_in > 0).astype(jnp.int32))
    earlier = jnp.sum(
        jnp.where(empty[None, :] & (target[None, :] < target[:, None]), 1, 0), axis=1
    )
    place = jnp.where(empty, filled + earlier + 128, slot_in - 1)
    modes = None
    for c in range(CHUNKS):
        modes = apply_inverse(place, weight, sent[c], modes, c * height, block)
    return (modes, operator)


def solution(mesh):
    placed = (
        P(AXES, None, None),
        P(AXES, None, None),
        P(AXES),
        P(),
        P(),
    )
    return jax.shard_map(
        body,
        mesh=mesh,
        in_specs=placed,
        out_specs=(P(AXES, None, None), P()),
        check_vma=False,
    )
```

```python
import functools

import jax
import jax.numpy as jnp
from jax import lax
from jax.experimental import pallas as pl
from jax.experimental.pallas import tpu as pltpu
from jax.sharding import PartitionSpec as P

AXES = ("rows", "grp")
GRAM_CHUNKS = (16, 32, 48)
PACK_CHUNKS = 4
APPLY_STEP = 16
NOTE_ROWS = 4
CAP = 128


def split_pair(x):
    hi = x.astype(jnp.bfloat16)
    lo = (x - hi.astype(jnp.float32)).astype(jnp.bfloat16)
    return hi, lo


def contract_rows(a, b):
    return lax.dot_general(
        a, b, (((0,), (0,)), ((), ())), preferred_element_type=jnp.float32
    )


def pack_kernel(dest_ref, late_ref, out_ref, buf, sem_in, sem_out):
    count = late_ref.shape[0]
    size = count // PACK_CHUNKS

    def load(t):
        part = pl.ds(t * size, size)
        return pltpu.make_async_copy(late_ref.at[part], buf.at[part], sem_in.at[t])

    for t in range(PACK_CHUNKS):
        load(t).start()
    for t in range(PACK_CHUNKS):
        load(t).wait()

        def send(i, carry):
            pltpu.make_async_copy(buf.at[i], out_ref.at[dest_ref[i]], sem_out).start()
            return carry

        lax.fori_loop(t * size, t * size + size, send, 0, unroll=8)
    pltpu.make_async_copy(buf, out_ref.at[pl.ds(0, count)], sem_out).wait()


def pack(late, dest, members):
    count, block, width = late.shape
    return pl.pallas_call(
        pack_kernel,
        grid_spec=pltpu.PrefetchScalarGridSpec(
            num_scalar_prefetch=1,
            grid=(1,),
            in_specs=[pl.BlockSpec(memory_space=pl.ANY)],
            out_specs=pl.BlockSpec(memory_space=pl.ANY),
            scratch_shapes=[
                pltpu.VMEM((count, block, width), jnp.float32),
                pltpu.SemaphoreType.DMA((PACK_CHUNKS,)),
                pltpu.SemaphoreType.DMA,
            ],
        ),
        out_shape=jax.ShapeDtypeStruct((members, block, width), jnp.float32),
        cost_estimate=pl.CostEstimate(flops=100000000, bytes_accessed=1 << 23, transcendentals=0),
        name="pack",
    )(dest, late)


def gram_kernel(early_ref, late_ref, out_ref, early_buf, late_buf, sem_early, sem_late):
    width = early_ref.shape[2]
    parts = []
    lo = 0
    for k, size in enumerate(GRAM_CHUNKS):
        part = pl.ds(lo, size)
        one = pltpu.make_async_copy(early_ref.at[part], early_buf.at[part], sem_early.at[k])
        two = pltpu.make_async_copy(late_ref.at[part], late_buf.at[part], sem_late.at[k])
        one.start()
        two.start()
        parts.append((part, one, two))
        lo += size
    gram_wide = cross_wide = None
    for part, one, two in parts:
        one.wait()
        two.wait()
        ehi, elo = split_pair(early_buf[part].reshape((-1, width)))
        lhi, llo = split_pair(late_buf[part].reshape((-1, width)))
        pair = jnp.concatenate([ehi, elo], axis=1)
        gram_part = contract_rows(ehi, pair)
        cross_part = contract_rows(pair, jnp.concatenate([lhi, llo], axis=1))
        gram_wide = gram_part if gram_wide is None else gram_wide + gram_part
        cross_wide = cross_part if cross_wide is None else cross_wide + cross_part
    mixed = gram_wide[:, width:]
    out_ref[:, 0, :] = gram_wide[:, 0:width] + (mixed + mixed.T)
    out_ref[:, 1, :] = cross_wide[0:width, 0:width] + (
        cross_wide[0:width, width:] + cross_wide[width:, 0:width]
    )


def gram_pair(early, late):
    count, block, width = early.shape
    steps = len(GRAM_CHUNKS)
    anywhere = pl.BlockSpec(memory_space=pl.ANY)
    return pl.pallas_call(
        gram_kernel,
        in_specs=[anywhere, anywhere],
        out_specs=pl.BlockSpec(memory_space=pltpu.VMEM),
        out_shape=jax.ShapeDtypeStruct((width, 2, width), jnp.float32),
        scratch_shapes=[
            pltpu.VMEM((count, block, width), jnp.float32),
            pltpu.VMEM((count, block, width), jnp.float32),
            pltpu.SemaphoreType.DMA((steps,)),
            pltpu.SemaphoreType.DMA((steps,)),
        ],
        cost_estimate=pl.CostEstimate(
            flops=12 * count * block * width * width, bytes_accessed=1 << 23, transcendentals=0
        ),
        name="gram",
    )(early, late)


def mix_kernel(partial_ref, note_ref, out_ref):
    members, _, width = partial_ref.shape
    gram_row = jnp.sum(partial_ref[:, 0, :], axis=0, keepdims=True)
    cross_row = jnp.sum(partial_ref[:, 1, :], axis=0, keepdims=True)
    out_ref[:, 0, :] = jnp.broadcast_to(gram_row, (members, width))
    out_ref[:, 1, :] = jnp.broadcast_to(cross_row, (members, width))
    out_ref[:, 2, :] = note_ref[...]
    out_ref[:, 3, :] = jnp.zeros((members, width), jnp.float32)


def mix(partial, note):
    members, _, width = partial.shape
    return pl.pallas_call(
        mix_kernel,
        out_shape=jax.ShapeDtypeStruct((members, NOTE_ROWS, width), jnp.float32),
        cost_estimate=pl.CostEstimate(flops=1000000, bytes_accessed=1 << 19, transcendentals=0),
        compiler_params=pltpu.CompilerParams(vmem_limit_bytes=4 << 20),
        name="mix",
    )(partial, note)


def dot3(a, b):
    return jnp.dot(a, b, precision=lax.Precision.HIGHEST, preferred_element_type=jnp.float32)


def finish_kernel(row_total, stats_ref, weight_ref, operator_ref, work):
    order = stats_ref.shape[0]
    row_id = lax.broadcasted_iota(jnp.int32, (order, 1), 0)
    lane = lax.broadcasted_iota(jnp.int32, (1, 2 * order), 1)
    lane_half = lax.broadcasted_iota(jnp.int32, (1, order), 1)
    work[:, 0:order] = stats_ref[:, 0, :] / row_total
    work[:, order:] = (row_id == lane_half).astype(jnp.float32)

    def step(j, carry):
        row = work[pl.ds(j, 1), :]
        inv = lax.rsqrt(jnp.sum(jnp.where(lane == j, row, 0.0), axis=1, keepdims=True))
        scaled = row * inv
        table = work[...]
        column = jnp.sum(
            jnp.where(lane_half == j, table[:, 0:order], 0.0), axis=1, keepdims=True
        )
        down = jnp.where(row_id > j, column * inv, 0.0)
        work[...] = jnp.where(row_id == j, scaled, table - down * scaled)
        return carry

    lax.fori_loop(0, order, step, 0)
    inverse_t = work[:, order:]
    inverse = inverse_t.T
    cross = stats_ref[:, 1, :] / row_total
    operator_ref[...] = dot3(inverse_t, dot3(cross, inverse))
    whi, wlo = split_pair(inverse)
    weight_ref[0:order, 0:order] = whi
    weight_ref[0:order, order:] = wlo
    weight_ref[order:, 0:order] = whi
    weight_ref[order:, order:] = wlo


def finish(stats, row_total):
    order = stats.shape[0]
    return pl.pallas_call(
        functools.partial(finish_kernel, float(row_total)),
        out_shape=(
            jax.ShapeDtypeStruct((2 * order, 2 * order), jnp.bfloat16),
            jax.ShapeDtypeStruct((order, order), jnp.float32),
        ),
        scratch_shapes=[pltpu.VMEM((order, 2 * order), jnp.float32)],
        cost_estimate=pl.CostEstimate(flops=1000000000, bytes_accessed=1 << 19, transcendentals=0),
        compiler_params=pltpu.CompilerParams(vmem_limit_bytes=4 << 20),
        name="finish",
    )(stats)


def apply_kernel(place_ref, weight_ref, arrived_ref, out_ref, buf_in, buf_out, sem_in, sem_out):
    count, block, width = arrived_ref.shape
    steps = count // APPLY_STEP

    def fetch(t):
        part = pl.ds(t * APPLY_STEP, APPLY_STEP)
        return pltpu.make_async_copy(arrived_ref.at[part], buf_in.at[part], sem_in.at[t])

    for t in range(steps):
        fetch(t).start()

    def step(t, carry):
        part = pl.ds(t * APPLY_STEP, APPLY_STEP)
        fetch(t).wait()
        hi, lo = split_pair(buf_in[part].reshape((APPLY_STEP * block, width)))
        wide = jnp.dot(
            jnp.concatenate([hi, lo], axis=1),
            weight_ref[...],
            preferred_element_type=jnp.float32,
        )
        solved = wide[:, 0:width] + wide[:, width:]
        buf_out[part] = solved.reshape((APPLY_STEP, block, width))
        for i in range(APPLY_STEP):
            row = t * APPLY_STEP + i
            code = place_ref[row]

            @pl.when(code >= count)
            def _():
                buf_out[row] = jnp.zeros((block, width), jnp.float32)

            pltpu.make_async_copy(
                buf_out.at[row], out_ref.at[lax.rem(code, count)], sem_out
            ).start()
        return carry

    lax.fori_loop(0, steps, step, 0)
    pltpu.make_async_copy(buf_out, out_ref, sem_out).wait()


def apply_inverse(place, weight, arrived):
    count, block, width = arrived.shape
    anywhere = pl.BlockSpec(memory_space=pl.ANY)
    return pl.pallas_call(
        apply_kernel,
        grid_spec=pltpu.PrefetchScalarGridSpec(
            num_scalar_prefetch=1,
            grid=(1,),
            in_specs=[pl.BlockSpec(memory_space=pltpu.VMEM), anywhere],
            out_specs=anywhere,
            scratch_shapes=[
                pltpu.VMEM((count, block, width), jnp.float32),
                pltpu.VMEM((count, block, width), jnp.float32),
                pltpu.SemaphoreType.DMA((count // APPLY_STEP,)),
                pltpu.SemaphoreType.DMA,
            ],
        ),
        out_shape=jax.ShapeDtypeStruct((count, block, width), jnp.float32),
        cost_estimate=pl.CostEstimate(
            flops=8 * count * block * width * width, bytes_accessed=1 << 23, transcendentals=0
        ),
        compiler_params=pltpu.CompilerParams(vmem_limit_bytes=24 << 20),
        name="apply",
    )(place, weight, arrived)


def exchange(payload):
    return lax.all_to_all(payload, AXES, split_axis=0, concat_axis=0, tiled=True)


def body(snap_early, snap_late, block_ids, block_owner, block_slot):
    members = lax.axis_size(AXES)
    count, block, width = snap_late.shape
    row_total = count * block * members
    outgoing = gram_pair(snap_early, snap_late)
    block_ids, outgoing = lax.optimization_barrier((block_ids, outgoing))
    partial = exchange(outgoing)
    labels = jnp.arange(block_owner.shape[0], dtype=jnp.int32)
    code = block_owner * CAP + block_slot
    hits = block_ids[:, None] == labels[None, :]
    code_here = jnp.sum(jnp.where(hits, code[None, :], 0), axis=1)
    dest = code_here // CAP
    slot_here = code_here % CAP
    target = jnp.arange(members, dtype=jnp.int32)
    note = jnp.sum(
        jnp.where(dest[None, :] == target[:, None], slot_here[None, :] + 1, 0), axis=1
    )
    note = jnp.broadcast_to(note.astype(jnp.float32)[:, None], (members, width))
    payload = pack(snap_late, dest, members)
    stats = exchange(mix(partial, note))
    payload, _ = lax.optimization_barrier((payload, stats))
    arrived = exchange(payload)
    weight, operator = finish(stats, row_total)
    slot_in = stats[:, 2, 0].astype(jnp.int32)
    empty = slot_in == 0
    filled = jnp.sum((slot_in > 0).astype(jnp.int32))
    earlier = jnp.sum(
        jnp.where(empty[None, :] & (target[None, :] < target[:, None]), 1, 0), axis=1
    )
    place = jnp.where(empty, filled + earlier + CAP, slot_in - 1)
    modes = apply_inverse(place, weight, arrived)
    return (modes, operator)


def solution(mesh):
    placed = (
        P(AXES, None, None),
        P(AXES, None, None),
        P(AXES),
        P(),
        P(),
    )
    return jax.shard_map(
        body,
        mesh=mesh,
        in_specs=placed,
        out_specs=(P(AXES, None, None), P()),
        check_vma=False,
    )
```

```python
import functools

import jax
import jax.numpy as jnp
from jax import lax
from jax.experimental import pallas as pl
from jax.experimental.pallas import tpu as pltpu
from jax.sharding import PartitionSpec as P

AXES = ("rows", "grp")
GRAM_CHUNKS = (16, 32, 48)
PACK_CHUNKS = 4
NOTE_ROWS = 8
LAST_ROWS = 16
CAP = 128


def split_pair(x):
    hi = x.astype(jnp.bfloat16)
    lo = (x - hi.astype(jnp.float32)).astype(jnp.bfloat16)
    return hi, lo


def contract_rows(a, b):
    return lax.dot_general(
        a, b, (((0,), (0,)), ((), ())), preferred_element_type=jnp.float32
    )


def pack_kernel(dest_ref, late_ref, first_ref, last_ref, buf, sem_in, sem_out, sem_last):
    count, block, _ = late_ref.shape
    size = count // PACK_CHUNKS
    last = last_ref.shape[1]
    first = block - last

    def load(t):
        part = pl.ds(t * size, size)
        return pltpu.make_async_copy(late_ref.at[part], buf.at[part], sem_in.at[t])

    for t in range(PACK_CHUNKS):
        load(t).start()
    for t in range(PACK_CHUNKS):
        load(t).wait()

        def send(i, carry):
            row = dest_ref[i]
            pltpu.make_async_copy(
                buf.at[i, pl.ds(0, first)], first_ref.at[row, pl.ds(0, first)], sem_out
            ).start()
            pltpu.make_async_copy(
                buf.at[i, pl.ds(first, last)], last_ref.at[row], sem_last
            ).start()
            return carry

        lax.fori_loop(t * size, t * size + size, send, 0, unroll=8)
    every = pl.ds(0, count)
    pltpu.make_async_copy(
        buf.at[:, pl.ds(0, first)], first_ref.at[every, pl.ds(0, first)], sem_out
    ).wait()
    pltpu.make_async_copy(buf.at[:, pl.ds(first, last)], last_ref.at[every], sem_last).wait()


def pack(late, dest, members):
    count, block, width = late.shape
    anywhere = pl.BlockSpec(memory_space=pl.ANY)
    first = block - LAST_ROWS
    return pl.pallas_call(
        pack_kernel,
        grid_spec=pltpu.PrefetchScalarGridSpec(
            num_scalar_prefetch=1,
            grid=(1,),
            in_specs=[anywhere],
            out_specs=(anywhere, anywhere),
            scratch_shapes=[
                pltpu.VMEM((count, block, width), jnp.float32),
                pltpu.SemaphoreType.DMA((PACK_CHUNKS,)),
                pltpu.SemaphoreType.DMA,
                pltpu.SemaphoreType.DMA,
            ],
        ),
        out_shape=(
            jax.ShapeDtypeStruct((members, first + NOTE_ROWS, width), jnp.float32),
            jax.ShapeDtypeStruct((members, LAST_ROWS, width), jnp.float32),
        ),
        cost_estimate=pl.CostEstimate(flops=100000000, bytes_accessed=1 << 23, transcendentals=0),
        name="pack",
    )(dest, late)


def gram_kernel(early_ref, late_ref, out_ref, early_buf, late_buf, sem_early, sem_late):
    width = early_ref.shape[2]
    parts = []
    lo = 0
    for k, size in enumerate(GRAM_CHUNKS):
        part = pl.ds(lo, size)
        one = pltpu.make_async_copy(early_ref.at[part], early_buf.at[part], sem_early.at[k])
        two = pltpu.make_async_copy(late_ref.at[part], late_buf.at[part], sem_late.at[k])
        one.start()
        two.start()
        parts.append((part, one, two))
        lo += size
    gram_wide = cross_wide = None
    for part, one, two in parts:
        one.wait()
        two.wait()
        ehi, elo = split_pair(early_buf[part].reshape((-1, width)))
        lhi, llo = split_pair(late_buf[part].reshape((-1, width)))
        pair = jnp.concatenate([ehi, elo], axis=1)
        gram_part = contract_rows(ehi, pair)
        cross_part = contract_rows(pair, jnp.concatenate([lhi, llo], axis=1))
        gram_wide = gram_part if gram_wide is None else gram_wide + gram_part
        cross_wide = cross_part if cross_wide is None else cross_wide + cross_part
    mixed = gram_wide[:, width:]
    out_ref[:, 0, :] = gram_wide[:, 0:width] + (mixed + mixed.T)
    out_ref[:, 1, :] = cross_wide[0:width, 0:width] + (
        cross_wide[0:width, width:] + cross_wide[width:, 0:width]
    )


def gram_pair(early, late):
    count, block, width = early.shape
    steps = len(GRAM_CHUNKS)
    anywhere = pl.BlockSpec(memory_space=pl.ANY)
    return pl.pallas_call(
        gram_kernel,
        in_specs=[anywhere, anywhere],
        out_specs=pl.BlockSpec(memory_space=pltpu.VMEM),
        out_shape=jax.ShapeDtypeStruct((width, 2, width), jnp.float32),
        scratch_shapes=[
            pltpu.VMEM((count, block, width), jnp.float32),
            pltpu.VMEM((count, block, width), jnp.float32),
            pltpu.SemaphoreType.DMA((steps,)),
            pltpu.SemaphoreType.DMA((steps,)),
        ],
        cost_estimate=pl.CostEstimate(
            flops=12 * count * block * width * width, bytes_accessed=1 << 23, transcendentals=0
        ),
        name="gram",
    )(early, late)


def mix_kernel(partial_ref, note_ref, first_ref, out_ref, rows, sem):
    members, _, width = partial_ref.shape
    gram_row = jnp.sum(partial_ref[:, 0, :], axis=0, keepdims=True)
    cross_row = jnp.sum(partial_ref[:, 1, :], axis=0, keepdims=True)
    rows[...] = jnp.zeros_like(rows)
    rows[:, 0, :] = jnp.broadcast_to(gram_row, (members, width))
    rows[:, 1, :] = jnp.broadcast_to(cross_row, (members, width))
    rows[:, 2, :] = note_ref[...]
    tail = pl.ds(out_ref.shape[1] - NOTE_ROWS, NOTE_ROWS)
    copy = pltpu.make_async_copy(rows, out_ref.at[:, tail], sem)
    copy.start()
    copy.wait()


def mix(partial, note, first):
    members, _, width = partial.shape
    whole = pl.BlockSpec(memory_space=pltpu.VMEM)
    anywhere = pl.BlockSpec(memory_space=pl.ANY)
    return pl.pallas_call(
        mix_kernel,
        in_specs=[whole, whole, anywhere],
        out_specs=anywhere,
        out_shape=jax.ShapeDtypeStruct(first.shape, first.dtype),
        scratch_shapes=[
            pltpu.VMEM((members, NOTE_ROWS, width), jnp.float32),
            pltpu.SemaphoreType.DMA,
        ],
        input_output_aliases={2: 0},
        cost_estimate=pl.CostEstimate(flops=1000000, bytes_accessed=1 << 19, transcendentals=0),
        compiler_params=pltpu.CompilerParams(vmem_limit_bytes=57 << 20),
        name="mix",
    )(partial, note, first)


def dot3(a, b):
    return jnp.dot(a, b, precision=lax.Precision.HIGHEST, preferred_element_type=jnp.float32)


def finish_kernel(row_total, arrived_ref, weight_ref, operator_ref, place_ref, work, stats_ref, sem):
    order = stats_ref.shape[0]
    tail = pl.ds(arrived_ref.shape[1] - NOTE_ROWS, NOTE_ROWS)
    copy = pltpu.make_async_copy(arrived_ref.at[:, tail], stats_ref, sem)
    copy.start()
    copy.wait()
    row_id = lax.broadcasted_iota(jnp.int32, (order, 1), 0)
    lane = lax.broadcasted_iota(jnp.int32, (1, 2 * order), 1)
    lane_half = lax.broadcasted_iota(jnp.int32, (1, order), 1)
    work[:, 0:order] = stats_ref[:, 0, :] / row_total
    work[:, order:] = (row_id == lane_half).astype(jnp.float32)

    def step(j, carry):
        row = work[pl.ds(j, 1), :]
        inv = lax.rsqrt(jnp.sum(jnp.where(lane == j, row, 0.0), axis=1, keepdims=True))
        scaled = row * inv
        table = work[...]
        column = jnp.sum(
            jnp.where(lane_half == j, table[:, 0:order], 0.0), axis=1, keepdims=True
        )
        down = jnp.where(row_id > j, column * inv, 0.0)
        work[...] = jnp.where(row_id == j, scaled, table - down * scaled)
        return carry

    lax.fori_loop(0, order, step, 0)
    inverse_t = work[:, order:]
    inverse = inverse_t.T
    cross = stats_ref[:, 1, :] / row_total
    operator_ref[...] = dot3(inverse_t, dot3(cross, inverse))
    whi, wlo = split_pair(inverse)
    weight_ref[0:order, 0:order] = whi
    weight_ref[0:order, order:] = wlo
    weight_ref[order:, 0:order] = whi
    weight_ref[order:, order:] = wlo
    note = stats_ref[:, 2, :]
    empty = note == 0.0
    counted = empty.astype(jnp.bfloat16)
    below = (row_id > lane_half).astype(jnp.bfloat16)
    earlier = jnp.dot(below, counted, preferred_element_type=jnp.float32)
    filled = order - jnp.sum(counted.astype(jnp.float32), axis=0, keepdims=True)
    code = jnp.where(empty, filled + earlier + CAP, note - 1.0)
    place_ref[...] = code.T[0:1, :].astype(jnp.int32)


def finish(arrived, row_total):
    order = arrived.shape[0]
    whole = pl.BlockSpec(memory_space=pltpu.VMEM)
    return pl.pallas_call(
        functools.partial(finish_kernel, float(row_total)),
        in_specs=[pl.BlockSpec(memory_space=pl.ANY)],
        out_specs=(whole, whole, whole),
        out_shape=(
            jax.ShapeDtypeStruct((2 * order, 2 * order), jnp.bfloat16),
            jax.ShapeDtypeStruct((order, order), jnp.float32),
            jax.ShapeDtypeStruct((1, order), jnp.int32),
        ),
        scratch_shapes=[
            pltpu.VMEM((order, 2 * order), jnp.float32),
            pltpu.VMEM((order, NOTE_ROWS, order), jnp.float32),
            pltpu.SemaphoreType.DMA,
        ],
        cost_estimate=pl.CostEstimate(flops=1000000000, bytes_accessed=1 << 19, transcendentals=0),
        compiler_params=pltpu.CompilerParams(vmem_limit_bytes=57 << 20),
        name="finish",
    )(arrived)


def apply_kernel(fast, stride, lo, height, place_ref, weight_ref, arrived_ref, *rest):
    if fast:
        out_ref, buf_out, sem_out = rest[-3:]
        buf_in = arrived_ref
    else:
        out_ref, buf_out, sem_out, buf_in, sem_in = rest[-5:]
    count, _, width = arrived_ref.shape
    steps = count // stride
    rows = pl.ds(lo, height)

    def fetch(t):
        part = pl.ds(t * stride, stride)
        return pltpu.make_async_copy(
            arrived_ref.at[part, pl.ds(0, height)], buf_in.at[part], sem_in.at[t]
        )

    if not fast:
        for t in range(steps):
            fetch(t).start()

    def step(t, carry):
        part = pl.ds(t * stride, stride)
        if not fast:
            fetch(t).wait()
        hi, low = split_pair(buf_in[part].reshape((stride * height, width)))
        wide = jnp.dot(
            jnp.concatenate([hi, low], axis=1),
            weight_ref[...],
            preferred_element_type=jnp.float32,
        )
        solved = wide[:, 0:width] + wide[:, width:]
        buf_out[part] = solved.reshape((stride, height, width))
        for i in range(stride):
            row = t * stride + i
            code = place_ref[row]

            @pl.when(code >= count)
            def _():
                buf_out[row] = jnp.zeros((height, width), jnp.float32)

            pltpu.make_async_copy(
                buf_out.at[row], out_ref.at[lax.rem(code, count), rows], sem_out
            ).start()
        return carry

    lax.fori_loop(0, steps, step, 0)
    pltpu.make_async_copy(buf_out, out_ref.at[:, rows], sem_out).wait()


def apply_inverse(place, weight, arrived, modes, stride, lo, height, block):
    count, _, width = arrived.shape
    anywhere = pl.BlockSpec(memory_space=pl.ANY)
    whole = pl.BlockSpec(memory_space=pltpu.VMEM)
    earlier = () if modes is None else (modes,)
    fast = modes is not None
    rows = pltpu.VMEM((count, height, width), jnp.float32)
    scratch = [rows, pltpu.SemaphoreType.DMA]
    if not fast:
        scratch += [rows, pltpu.SemaphoreType.DMA((count // stride,))]
    return pl.pallas_call(
        functools.partial(apply_kernel, fast, stride, lo, height),
        grid_spec=pltpu.PrefetchScalarGridSpec(
            num_scalar_prefetch=1,
            grid=(1,),
            in_specs=[whole, whole if fast else anywhere] + [anywhere] * len(earlier),
            out_specs=anywhere,
            scratch_shapes=scratch,
        ),
        out_shape=jax.ShapeDtypeStruct((count, block, width), jnp.float32),
        input_output_aliases={3: 0} if earlier else {},
        cost_estimate=pl.CostEstimate(
            flops=8 * count * height * width * width, bytes_accessed=1 << 23, transcendentals=0
        ),
        compiler_params=pltpu.CompilerParams(vmem_limit_bytes=(4 if fast else 57) << 20),
        name="apply",
    )(place, weight, arrived, *earlier)


def exchange(payload):
    return lax.all_to_all(payload, AXES, split_axis=0, concat_axis=0, tiled=True)


def body(snap_early, snap_late, block_ids, block_owner, block_slot):
    members = lax.axis_size(AXES)
    count, block, width = snap_late.shape
    row_total = count * block * members
    outgoing = gram_pair(snap_early, snap_late)
    block_ids, outgoing = lax.optimization_barrier((block_ids, outgoing))
    partial = exchange(outgoing)
    labels = jnp.arange(block_owner.shape[0], dtype=jnp.int32)
    code = block_owner * CAP + block_slot
    hits = block_ids[:, None] == labels[None, :]
    code_here = jnp.sum(jnp.where(hits, code[None, :], 0), axis=1)
    dest = code_here // CAP
    slot_here = code_here % CAP
    target = jnp.arange(members, dtype=jnp.int32)
    note = jnp.sum(
        jnp.where(dest[None, :] == target[:, None], slot_here[None, :] + 1, 0), axis=1
    )
    note = jnp.broadcast_to(note.astype(jnp.float32)[:, None], (members, width))
    first, last = pack(snap_late, dest, members)
    first = exchange(mix(partial, note, first))
    last, first = lax.optimization_barrier((last, first))
    last = exchange(last)
    weight, operator, place = finish(first, row_total)
    place = place.reshape((members,))
    height = block - LAST_ROWS
    modes = apply_inverse(place, weight, first, None, 16, 0, height, block)
    modes = apply_inverse(place, weight, last, modes, 64, height, LAST_ROWS, block)
    return (modes, operator)


def solution(mesh):
    placed = (
        P(AXES, None, None),
        P(AXES, None, None),
        P(AXES),
        P(),
        P(),
    )
    return jax.shard_map(
        body,
        mesh=mesh,
        in_specs=placed,
        out_specs=(P(AXES, None, None), P()),
        check_vma=False,
    )
```

```python
import functools

import jax
import jax.numpy as jnp
from jax import lax
from jax.experimental import pallas as pl
from jax.experimental.pallas import tpu as pltpu
from jax.sharding import PartitionSpec as P

AXES = ("y", "x", "z", "core")
PLANE = ("x", "z", "core")
GRAM_CHUNKS = (16, 32, 48)
PACK_CHUNKS = 4
SUM_ROWS = 8
LAST_ROWS = 32
CAP = 128


def split_pair(x):
    hi = x.astype(jnp.bfloat16)
    lo = (x - hi.astype(jnp.float32)).astype(jnp.bfloat16)
    return hi, lo


def contract_rows(a, b):
    return lax.dot_general(
        a, b, (((0,), (0,)), ((), ())), preferred_element_type=jnp.float32
    )


def pack_kernel(lo, height, dest_ref, late_ref, out_ref, buf, sem_in, sem_out):
    count = late_ref.shape[0]
    size = count // PACK_CHUNKS
    rows = pl.ds(0, height)

    def load(t):
        part = pl.ds(t * size, size)
        return pltpu.make_async_copy(
            late_ref.at[part, pl.ds(lo, height)], buf.at[part], sem_in.at[t]
        )

    for t in range(PACK_CHUNKS):
        load(t).start()
    for t in range(PACK_CHUNKS):
        load(t).wait()

        def send(i, carry):
            pltpu.make_async_copy(buf.at[i], out_ref.at[dest_ref[i], rows], sem_out).start()
            return carry

        lax.fori_loop(t * size, t * size + size, send, 0, unroll=8)
    pltpu.make_async_copy(buf, out_ref.at[pl.ds(0, count), rows], sem_out).wait()


def pack(late, dest, members, lo, height, spare):
    count, _, width = late.shape
    anywhere = pl.BlockSpec(memory_space=pl.ANY)
    return pl.pallas_call(
        functools.partial(pack_kernel, lo, height),
        grid_spec=pltpu.PrefetchScalarGridSpec(
            num_scalar_prefetch=1,
            grid=(1,),
            in_specs=[anywhere],
            out_specs=anywhere,
            scratch_shapes=[
                pltpu.VMEM((count, height, width), jnp.float32),
                pltpu.SemaphoreType.DMA((PACK_CHUNKS,)),
                pltpu.SemaphoreType.DMA,
            ],
        ),
        out_shape=jax.ShapeDtypeStruct((members, height + spare, width), jnp.float32),
        cost_estimate=pl.CostEstimate(flops=100000000, bytes_accessed=1 << 23, transcendentals=0),
        name="pack",
    )(dest, late)


def gram_kernel(early_ref, late_ref, out_ref, early_buf, late_buf, sem_early, sem_late):
    width = early_ref.shape[2]
    parts = []
    lo = 0
    for k, size in enumerate(GRAM_CHUNKS):
        part = pl.ds(lo, size)
        one = pltpu.make_async_copy(early_ref.at[part], early_buf.at[part], sem_early.at[k])
        two = pltpu.make_async_copy(late_ref.at[part], late_buf.at[part], sem_late.at[k])
        one.start()
        two.start()
        parts.append((part, one, two))
        lo += size
    gram_wide = cross_wide = None
    for part, one, two in parts:
        one.wait()
        two.wait()
        ehi, elo = split_pair(early_buf[part].reshape((-1, width)))
        lhi, llo = split_pair(late_buf[part].reshape((-1, width)))
        pair = jnp.concatenate([ehi, elo], axis=1)
        gram_part = contract_rows(ehi, pair)
        cross_part = contract_rows(pair, jnp.concatenate([lhi, llo], axis=1))
        gram_wide = gram_part if gram_wide is None else gram_wide + gram_part
        cross_wide = cross_part if cross_wide is None else cross_wide + cross_part
    mixed = gram_wide[:, width:]
    gram = gram_wide[:, 0:width] + (mixed + mixed.T)
    cross = cross_wide[0:width, 0:width] + (
        cross_wide[0:width, width:] + cross_wide[width:, 0:width]
    )
    size = out_ref.shape[0]
    half = SUM_ROWS // 2
    for r in range(half):
        out_ref[:, r, :] = gram[r * size : (r + 1) * size, :]
        out_ref[:, half + r, :] = cross[r * size : (r + 1) * size, :]


def gram_pair(early, late):
    count, block, width = early.shape
    steps = len(GRAM_CHUNKS)
    anywhere = pl.BlockSpec(memory_space=pl.ANY)
    return pl.pallas_call(
        gram_kernel,
        in_specs=[anywhere, anywhere],
        out_specs=pl.BlockSpec(memory_space=pltpu.VMEM),
        out_shape=jax.ShapeDtypeStruct((2 * width // SUM_ROWS, SUM_ROWS, width), jnp.float32),
        scratch_shapes=[
            pltpu.VMEM((count, block, width), jnp.float32),
            pltpu.VMEM((count, block, width), jnp.float32),
            pltpu.SemaphoreType.DMA((steps,)),
            pltpu.SemaphoreType.DMA((steps,)),
        ],
        cost_estimate=pl.CostEstimate(
            flops=12 * count * block * width * width, bytes_accessed=1 << 23, transcendentals=0
        ),
        name="gram",
    )(early, late)


def mix_kernel(partial_ref, note_ref, first_ref, out_ref, rows, sem):
    members, _, width = rows.shape
    total = jnp.sum(partial_ref[...], axis=0, keepdims=True)
    rows[...] = jnp.broadcast_to(total, rows.shape)
    mark = SUM_ROWS // 2 - 1
    lane = lax.broadcasted_iota(jnp.int32, (members, width), 1)
    rows[:, mark, :] = jnp.where(lane == 0, note_ref[...], total[0, mark : mark + 1, :])
    tail = pl.ds(out_ref.shape[1] - SUM_ROWS, SUM_ROWS)
    copy = pltpu.make_async_copy(rows, out_ref.at[:, tail], sem)
    copy.start()
    copy.wait()


def mix(partial, note, first):
    members, _, width = first.shape
    whole = pl.BlockSpec(memory_space=pltpu.VMEM)
    anywhere = pl.BlockSpec(memory_space=pl.ANY)
    return pl.pallas_call(
        mix_kernel,
        in_specs=[whole, whole, anywhere],
        out_specs=anywhere,
        out_shape=jax.ShapeDtypeStruct(first.shape, first.dtype),
        scratch_shapes=[
            pltpu.VMEM((members, SUM_ROWS, width), jnp.float32),
            pltpu.SemaphoreType.DMA,
        ],
        input_output_aliases={2: 0},
        cost_estimate=pl.CostEstimate(flops=1000000, bytes_accessed=1 << 19, transcendentals=0),
        compiler_params=pltpu.CompilerParams(vmem_limit_bytes=57 << 20),
        name="mix",
    )(partial, note, first)


def dot3(a, b):
    return jnp.dot(a, b, precision=lax.Precision.HIGHEST, preferred_element_type=jnp.float32)


def finish_kernel(row_total, arrived_ref, weight_ref, operator_ref, place_ref, work, stats_ref, sem):
    order = stats_ref.shape[0]
    tail = pl.ds(arrived_ref.shape[1] - SUM_ROWS, SUM_ROWS)
    copy = pltpu.make_async_copy(arrived_ref.at[:, tail], stats_ref, sem)
    copy.start()
    copy.wait()
    row_id = lax.broadcasted_iota(jnp.int32, (order, 1), 0)
    lane = lax.broadcasted_iota(jnp.int32, (1, 2 * order), 1)
    lane_half = lax.broadcasted_iota(jnp.int32, (1, order), 1)
    size = 2 * order // SUM_ROWS
    half = SUM_ROWS // 2
    note = stats_ref[:, half - 1, 0:1]
    total = stats_ref[0:size]
    for p in range(1, order // size):
        total = total + stats_ref[p * size : (p + 1) * size]
    gram = jnp.concatenate([total[:, r, :] for r in range(half)], axis=0)
    cross = jnp.concatenate([total[:, half + r, :] for r in range(half)], axis=0) / row_total
    work[:, 0:order] = jnp.where(row_id > lane_half, gram.T, gram) / row_total
    work[:, order:] = (row_id == lane_half).astype(jnp.float32)

    def step(j, carry):
        row = work[pl.ds(j, 1), :]
        inv = lax.rsqrt(jnp.sum(jnp.where(lane == j, row, 0.0), axis=1, keepdims=True))
        scaled = row * inv
        table = work[...]
        column = jnp.sum(
            jnp.where(lane_half == j, table[:, 0:order], 0.0), axis=1, keepdims=True
        )
        down = jnp.where(row_id > j, column * inv, 0.0)
        work[...] = jnp.where(row_id == j, scaled, table - down * scaled)
        return carry

    lax.fori_loop(0, order, step, 0)
    inverse_t = work[:, order:]
    inverse = inverse_t.T
    operator_ref[...] = dot3(inverse_t, dot3(cross, inverse))
    whi, wlo = split_pair(inverse)
    weight_ref[0:order, 0:order] = whi
    weight_ref[0:order, order:] = wlo
    weight_ref[order:, 0:order] = whi
    weight_ref[order:, order:] = wlo
    note = jnp.broadcast_to(note, (order, order))
    empty = note == 0.0
    counted = empty.astype(jnp.bfloat16)
    below = (row_id > lane_half).astype(jnp.bfloat16)
    earlier = jnp.dot(below, counted, preferred_element_type=jnp.float32)
    filled = order - jnp.sum(counted.astype(jnp.float32), axis=0, keepdims=True)
    code = jnp.where(empty, filled + earlier + CAP, note - 1.0)
    place_ref[...] = code.T[0:1, :].astype(jnp.int32)


def finish(arrived, row_total):
    order = arrived.shape[0]
    whole = pl.BlockSpec(memory_space=pltpu.VMEM)
    return pl.pallas_call(
        functools.partial(finish_kernel, float(row_total)),
        in_specs=[pl.BlockSpec(memory_space=pl.ANY)],
        out_specs=(whole, whole, whole),
        out_shape=(
            jax.ShapeDtypeStruct((2 * order, 2 * order), jnp.bfloat16),
            jax.ShapeDtypeStruct((order, order), jnp.float32),
            jax.ShapeDtypeStruct((1, order), jnp.int32),
        ),
        scratch_shapes=[
            pltpu.VMEM((order, 2 * order), jnp.float32),
            pltpu.VMEM((order, SUM_ROWS, order), jnp.float32),
            pltpu.SemaphoreType.DMA,
        ],
        cost_estimate=pl.CostEstimate(flops=1000000000, bytes_accessed=1 << 19, transcendentals=0),
        compiler_params=pltpu.CompilerParams(vmem_limit_bytes=57 << 20),
        name="finish",
    )(arrived)


def apply_kernel(fast, stride, lo, height, place_ref, weight_ref, arrived_ref, *rest):
    if fast:
        out_ref, buf_out, sem_out = rest[-3:]
        buf_in = arrived_ref
    else:
        out_ref, buf_out, sem_out, buf_in, sem_in = rest[-5:]
    count, _, width = arrived_ref.shape
    steps = count // stride
    rows = pl.ds(lo, height)

    def fetch(t):
        part = pl.ds(t * stride, stride)
        return pltpu.make_async_copy(
            arrived_ref.at[part, pl.ds(0, height)], buf_in.at[part], sem_in.at[t]
        )

    if not fast:
        for t in range(steps):
            fetch(t).start()

    def step(t, carry):
        part = pl.ds(t * stride, stride)
        if not fast:
            fetch(t).wait()
        hi, low = split_pair(buf_in[part].reshape((stride * height, width)))
        wide = jnp.dot(
            jnp.concatenate([hi, low], axis=1),
            weight_ref[...],
            preferred_element_type=jnp.float32,
        )
        solved = wide[:, 0:width] + wide[:, width:]
        buf_out[part] = solved.reshape((stride, height, width))
        for i in range(stride):
            row = t * stride + i
            code = place_ref[row]

            @pl.when(code >= count)
            def _():
                buf_out[row] = jnp.zeros((height, width), jnp.float32)

            pltpu.make_async_copy(
                buf_out.at[row], out_ref.at[lax.rem(code, count), rows], sem_out
            ).start()
        return carry

    lax.fori_loop(0, steps, step, 0)
    pltpu.make_async_copy(buf_out, out_ref.at[:, rows], sem_out).wait()


def apply_inverse(place, weight, arrived, modes, stride, lo, height, block):
    count, _, width = arrived.shape
    anywhere = pl.BlockSpec(memory_space=pl.ANY)
    whole = pl.BlockSpec(memory_space=pltpu.VMEM)
    earlier = () if modes is None else (modes,)
    fast = modes is not None
    rows = pltpu.VMEM((count, height, width), jnp.float32)
    scratch = [rows, pltpu.SemaphoreType.DMA]
    if not fast:
        scratch += [rows, pltpu.SemaphoreType.DMA((count // stride,))]
    return pl.pallas_call(
        functools.partial(apply_kernel, fast, stride, lo, height),
        grid_spec=pltpu.PrefetchScalarGridSpec(
            num_scalar_prefetch=1,
            grid=(1,),
            in_specs=[whole, whole if fast else anywhere] + [anywhere] * len(earlier),
            out_specs=anywhere,
            scratch_shapes=scratch,
        ),
        out_shape=jax.ShapeDtypeStruct((count, block, width), jnp.float32),
        input_output_aliases={3: 0} if earlier else {},
        cost_estimate=pl.CostEstimate(
            flops=8 * count * height * width * width, bytes_accessed=1 << 23, transcendentals=0
        ),
        compiler_params=pltpu.CompilerParams(vmem_limit_bytes=(4 if fast else 57) << 20),
        name="apply",
    )(place, weight, arrived, *earlier)


def exchange(payload, axes=AXES):
    return lax.all_to_all(payload, axes, split_axis=0, concat_axis=0, tiled=True)


def body(snap_early, snap_late, block_ids, block_owner, block_slot):
    members = lax.axis_size(AXES)
    count, block, width = snap_late.shape
    row_total = count * block * members
    outgoing = gram_pair(snap_early, snap_late)
    block_ids, outgoing = lax.optimization_barrier((block_ids, outgoing))
    partial = exchange(outgoing, PLANE)
    labels = jnp.arange(block_owner.shape[0], dtype=jnp.int32)
    code = block_owner * CAP + block_slot
    hits = block_ids[:, None] == labels[None, :]
    code_here = jnp.sum(jnp.where(hits, code[None, :], 0), axis=1)
    dest = code_here // CAP
    slot_here = code_here % CAP
    target = jnp.arange(members, dtype=jnp.int32)
    note = jnp.sum(
        jnp.where(dest[None, :] == target[:, None], slot_here[None, :] + 1, 0), axis=1
    )
    note = jnp.broadcast_to(note.astype(jnp.float32)[:, None], (members, width))
    height = block - LAST_ROWS
    first = pack(snap_late, dest, members, 0, height, SUM_ROWS)
    first = mix(partial, note, first)
    dest, first = lax.optimization_barrier((dest, first))
    first = exchange(first)
    last = pack(snap_late, dest, members, height, LAST_ROWS, 0)
    last, first = lax.optimization_barrier((last, first))
    last = exchange(last)
    weight, operator, place = finish(first, row_total)
    place = place.reshape((members,))
    modes = apply_inverse(place, weight, first, None, 16, 0, height, block)
    modes = apply_inverse(place, weight, last, modes, 64, height, LAST_ROWS, block)
    return (modes, operator)


def solution(mesh):
    split = jax.sharding.Mesh(mesh.devices.reshape((4, 4, 4, 2)), AXES)
    placed = (
        P(AXES, None, None),
        P(AXES, None, None),
        P(AXES),
        P(),
        P(),
    )
    return jax.shard_map(
        body,
        mesh=split,
        in_specs=placed,
        out_specs=(P(AXES, None, None), P()),
        check_vma=False,
    )
```

```python
import functools

import jax
import jax.numpy as jnp
from jax import lax
from jax.experimental import pallas as pl
from jax.experimental.pallas import tpu as pltpu
from jax.sharding import PartitionSpec as P

AXES = ("y", "x", "z", "core")
PLANE = ("x", "z", "core")
GRAM_CHUNKS = (16, 32, 48)
PACK_CHUNKS = 4
APPLY_STEP = 16
SUM_ROWS = 8
PIVOTS = 4
SHRINK = 32
CAP = 128


def split_pair(x):
    hi = x.astype(jnp.bfloat16)
    lo = (x - hi.astype(jnp.float32)).astype(jnp.bfloat16)
    return hi, lo


def contract_rows(a, b):
    return lax.dot_general(
        a, b, (((0,), (0,)), ((), ())), preferred_element_type=jnp.float32
    )


def pack_kernel(lo, height, dest_ref, late_ref, out_ref, buf, sem_in, sem_out):
    count = late_ref.shape[0]
    size = count // PACK_CHUNKS
    rows = pl.ds(0, height)

    def load(t):
        part = pl.ds(t * size, size)
        return pltpu.make_async_copy(
            late_ref.at[part, pl.ds(lo, height)], buf.at[part], sem_in.at[t]
        )

    for t in range(PACK_CHUNKS):
        load(t).start()
    for t in range(PACK_CHUNKS):
        load(t).wait()

        def send(i, carry):
            pltpu.make_async_copy(buf.at[i], out_ref.at[dest_ref[i], rows], sem_out).start()
            return carry

        lax.fori_loop(t * size, t * size + size, send, 0, unroll=8)
    pltpu.make_async_copy(buf, out_ref.at[pl.ds(0, count), rows], sem_out).wait()


def pack(late, dest, members, lo, height, spare):
    count, _, width = late.shape
    anywhere = pl.BlockSpec(memory_space=pl.ANY)
    return pl.pallas_call(
        functools.partial(pack_kernel, lo, height),
        grid_spec=pltpu.PrefetchScalarGridSpec(
            num_scalar_prefetch=1,
            grid=(1,),
            in_specs=[anywhere],
            out_specs=anywhere,
            scratch_shapes=[
                pltpu.VMEM((count, height, width), jnp.float32),
                pltpu.SemaphoreType.DMA((PACK_CHUNKS,)),
                pltpu.SemaphoreType.DMA,
            ],
        ),
        out_shape=jax.ShapeDtypeStruct((members, height + spare, width), jnp.float32),
        cost_estimate=pl.CostEstimate(flops=100000000, bytes_accessed=1 << 23, transcendentals=0),
        name="pack",
    )(dest, late)


def gram_kernel(early_ref, late_ref, out_ref, early_buf, late_buf, sem_early, sem_late):
    width = early_ref.shape[2]
    parts = []
    lo = 0
    for k, size in enumerate(GRAM_CHUNKS):
        part = pl.ds(lo, size)
        one = pltpu.make_async_copy(early_ref.at[part], early_buf.at[part], sem_early.at[k])
        two = pltpu.make_async_copy(late_ref.at[part], late_buf.at[part], sem_late.at[k])
        one.start()
        two.start()
        parts.append((part, one, two))
        lo += size
    gram_wide = cross_wide = None
    for part, one, two in parts:
        one.wait()
        two.wait()
        ehi, elo = split_pair(early_buf[part].reshape((-1, width)))
        lhi, llo = split_pair(late_buf[part].reshape((-1, width)))
        pair = jnp.concatenate([ehi, elo], axis=1)
        gram_part = contract_rows(ehi, pair)
        cross_part = contract_rows(pair, jnp.concatenate([lhi, llo], axis=1))
        gram_wide = gram_part if gram_wide is None else gram_wide + gram_part
        cross_wide = cross_part if cross_wide is None else cross_wide + cross_part
    mixed = gram_wide[:, width:]
    gram = gram_wide[:, 0:width] + (mixed + mixed.T)
    cross = cross_wide[0:width, 0:width] + (
        cross_wide[0:width, width:] + cross_wide[width:, 0:width]
    )
    size = out_ref.shape[0]
    half = SUM_ROWS // 2
    for r in range(half):
        out_ref[:, r, :] = gram[r * size : (r + 1) * size, :]
        out_ref[:, half + r, :] = cross[r * size : (r + 1) * size, :]


def gram_pair(early, late):
    count, block, width = early.shape
    steps = len(GRAM_CHUNKS)
    anywhere = pl.BlockSpec(memory_space=pl.ANY)
    return pl.pallas_call(
        gram_kernel,
        in_specs=[anywhere, anywhere],
        out_specs=pl.BlockSpec(memory_space=pltpu.VMEM),
        out_shape=jax.ShapeDtypeStruct((2 * width // SUM_ROWS, SUM_ROWS, width), jnp.float32),
        scratch_shapes=[
            pltpu.VMEM((count, block, width), jnp.float32),
            pltpu.VMEM((count, block, width), jnp.float32),
            pltpu.SemaphoreType.DMA((steps,)),
            pltpu.SemaphoreType.DMA((steps,)),
        ],
        cost_estimate=pl.CostEstimate(
            flops=12 * count * block * width * width, bytes_accessed=1 << 23, transcendentals=0
        ),
        name="gram",
    )(early, late)


def mix_kernel(partial_ref, code_ref, first_ref, out_ref, rows, sem):
    members, _, width = rows.shape
    total = jnp.sum(partial_ref[...], axis=0, keepdims=True)
    rows[...] = jnp.broadcast_to(total, rows.shape)
    mark = SUM_ROWS // 2 - 1
    code = code_ref[...]
    peer = lax.broadcasted_iota(jnp.int32, (members, code.shape[1]), 0)
    slot = (jnp.bitwise_and(code, CAP - 1) + 1).astype(jnp.float32)
    here = jnp.where(jnp.right_shift(code, 7) == peer, slot, 0.0)
    note = jnp.sum(here, axis=1, keepdims=True)
    lane = lax.broadcasted_iota(jnp.int32, (members, width), 1)
    rows[:, mark, :] = jnp.where(lane == 0, note, total[0, mark : mark + 1, :])
    tail = pl.ds(out_ref.shape[1] - SUM_ROWS, SUM_ROWS)
    copy = pltpu.make_async_copy(rows, out_ref.at[:, tail], sem)
    copy.start()
    copy.wait()


def mix(partial, code, first):
    members, _, width = first.shape
    whole = pl.BlockSpec(memory_space=pltpu.VMEM)
    anywhere = pl.BlockSpec(memory_space=pl.ANY)
    return pl.pallas_call(
        mix_kernel,
        in_specs=[whole, whole, anywhere],
        out_specs=anywhere,
        out_shape=jax.ShapeDtypeStruct(first.shape, first.dtype),
        scratch_shapes=[
            pltpu.VMEM((members, SUM_ROWS, width), jnp.float32),
            pltpu.SemaphoreType.DMA,
        ],
        input_output_aliases={2: 0},
        cost_estimate=pl.CostEstimate(flops=1000000, bytes_accessed=1 << 19, transcendentals=0),
        compiler_params=pltpu.CompilerParams(vmem_limit_bytes=57 << 20),
        name="mix",
    )(partial, code, first)


def dot3(a, b):
    return jnp.dot(a, b, precision=lax.Precision.HIGHEST, preferred_element_type=jnp.float32)


def eliminate(work):
    order = work.shape[0]
    lane = lax.broadcasted_iota(jnp.int32, (1, 2 * order), 1)
    lane_half = lax.broadcasted_iota(jnp.int32, (1, order), 1)

    def step(lo, k, carry):
        j = lo + k * PIVOTS
        row_id = lo + lax.broadcasted_iota(jnp.int32, (order - lo, 1), 0)
        table = work[lo:order, :]
        left = table[:, 0:order]
        rows = []
        columns = []
        for p in range(PIVOTS):
            rows.append(work[pl.ds(j + p, 1), :])
            picked = jnp.where(lane_half == j + p, left, 0.0)
            columns.append(jnp.sum(picked, axis=1, keepdims=True))
        block = {}
        for p in range(PIVOTS):
            for q in range(p, PIVOTS):
                picked = jnp.where(lane == j + q, rows[p], 0.0)
                block[p, q] = jnp.sum(picked, axis=1, keepdims=True)
        upper = {}
        for p in range(PIVOTS):
            pivot = block[p, p]
            for m in range(p):
                pivot = pivot - upper[m, p] * upper[m, p]
            inv = lax.rsqrt(pivot)
            for q in range(p + 1, PIVOTS):
                entry = block[p, q]
                for m in range(p):
                    entry = entry - upper[m, p] * upper[m, q]
                upper[p, q] = entry * inv
            for m in range(p):
                rows[p] = rows[p] - upper[m, p] * rows[m]
                columns[p] = columns[p] - upper[m, p] * columns[m]
            rows[p] = rows[p] * inv
            columns[p] = columns[p] * inv
        below = row_id >= j + PIVOTS
        for p in range(PIVOTS):
            table = table - jnp.where(below, columns[p], 0.0) * rows[p]
        for p in range(PIVOTS):
            table = jnp.where(row_id == j + p, rows[p], table)
        work[lo:order, :] = table
        return carry

    for lo in range(0, order, SHRINK):
        lax.fori_loop(0, SHRINK // PIVOTS, functools.partial(step, lo), 0)


def settle_kernel(
    row_total,
    arrived_ref,
    modes_ref,
    operator_ref,
    buf_in,
    buf_out,
    stats_ref,
    work,
    weight_ref,
    place_ref,
    slots_ref,
    sem_stats,
    sem_in,
    sem_out,
    sem_place,
):
    count, block, width = modes_ref.shape
    order = width
    steps = count // APPLY_STEP
    stats_copy = pltpu.make_async_copy(
        arrived_ref.at[:, pl.ds(block, SUM_ROWS)], stats_ref, sem_stats
    )
    stats_copy.start()

    def fetch(t):
        part = pl.ds(t * APPLY_STEP, APPLY_STEP)
        return pltpu.make_async_copy(
            arrived_ref.at[part, pl.ds(0, block)], buf_in.at[part], sem_in.at[t]
        )

    for t in range(steps):
        fetch(t).start()
    stats_copy.wait()

    row_id = lax.broadcasted_iota(jnp.int32, (order, 1), 0)
    lane = lax.broadcasted_iota(jnp.int32, (1, order), 1)
    size = 2 * order // SUM_ROWS
    half = SUM_ROWS // 2
    total = stats_ref[0:size]
    for p in range(1, order // size):
        total = total + stats_ref[p * size : (p + 1) * size]
    gram = jnp.concatenate([total[:, r, :] for r in range(half)], axis=0)
    work[:, 0:order] = jnp.where(row_id > lane, gram.T, gram) / row_total
    work[:, order:] = (row_id == lane).astype(jnp.float32)

    note = jnp.broadcast_to(stats_ref[:, half - 1, 0:1], (count, count))
    empty = note == 0.0
    counted = empty.astype(jnp.bfloat16)
    below = (row_id > lane).astype(jnp.bfloat16)
    earlier = jnp.dot(below, counted, preferred_element_type=jnp.float32)
    filled = count - jnp.sum(counted.astype(jnp.float32), axis=0, keepdims=True)
    code = jnp.where(empty, filled + earlier + CAP, note - 1.0)
    place_ref[...] = code.T[0:1, :].astype(jnp.int32)
    place_copy = pltpu.make_async_copy(place_ref, slots_ref, sem_place)
    place_copy.start()

    eliminate(work)
    inverse_t = work[:, order:]
    inverse = inverse_t.T
    whi, wlo = split_pair(inverse)
    weight_ref[0:order, 0:order] = whi
    weight_ref[0:order, order:] = wlo
    weight_ref[order:, 0:order] = whi
    weight_ref[order:, order:] = wlo
    place_copy.wait()

    def step(t, carry):
        part = pl.ds(t * APPLY_STEP, APPLY_STEP)
        fetch(t).wait()
        hi, low = split_pair(buf_in[part].reshape((APPLY_STEP * block, width)))
        wide = jnp.dot(
            jnp.concatenate([hi, low], axis=1),
            weight_ref[...],
            preferred_element_type=jnp.float32,
        )
        solved = wide[:, 0:width] + wide[:, width:]
        buf_out[part] = solved.reshape((APPLY_STEP, block, width))
        for i in range(APPLY_STEP):
            row = t * APPLY_STEP + i
            slot = slots_ref[0, row]

            @pl.when(slot >= CAP)
            def _():
                buf_out[row] = jnp.zeros((block, width), jnp.float32)

            pltpu.make_async_copy(
                buf_out.at[row], modes_ref.at[jnp.bitwise_and(slot, CAP - 1)], sem_out
            ).start()
        return carry

    lax.fori_loop(0, steps, step, 0)
    cross = jnp.concatenate([total[:, half + r, :] for r in range(half)], axis=0) / row_total
    operator_ref[...] = dot3(inverse_t, dot3(cross, inverse))
    pltpu.make_async_copy(buf_out, modes_ref, sem_out).wait()


def settle(arrived, row_total, block):
    count, _, width = arrived.shape
    anywhere = pl.BlockSpec(memory_space=pl.ANY)
    rows = pltpu.VMEM((count, block, width), jnp.float32)
    return pl.pallas_call(
        functools.partial(settle_kernel, float(row_total)),
        in_specs=[anywhere],
        out_specs=(anywhere, pl.BlockSpec(memory_space=pltpu.VMEM)),
        out_shape=(
            jax.ShapeDtypeStruct((count, block, width), jnp.float32),
            jax.ShapeDtypeStruct((width, width), jnp.float32),
        ),
        scratch_shapes=[
            rows,
            rows,
            pltpu.VMEM((count, SUM_ROWS, width), jnp.float32),
            pltpu.VMEM((width, 2 * width), jnp.float32),
            pltpu.VMEM((2 * width, 2 * width), jnp.bfloat16),
            pltpu.VMEM((1, count), jnp.int32),
            pltpu.SMEM((1, count), jnp.int32),
            pltpu.SemaphoreType.DMA,
            pltpu.SemaphoreType.DMA((count // APPLY_STEP,)),
            pltpu.SemaphoreType.DMA,
            pltpu.SemaphoreType.DMA,
        ],
        cost_estimate=pl.CostEstimate(
            flops=8 * count * block * width * width, bytes_accessed=1 << 23, transcendentals=0
        ),
        name="settle",
    )(arrived)


def exchange(payload, axes=AXES):
    return lax.all_to_all(payload, axes, split_axis=0, concat_axis=0, tiled=True)


def body(snap_early, snap_late, block_ids, block_owner, block_slot):
    members = lax.axis_size(AXES)
    count, block, width = snap_late.shape
    row_total = count * block * members
    outgoing = gram_pair(snap_early, snap_late)
    block_ids, outgoing = lax.optimization_barrier((block_ids, outgoing))
    partial = exchange(outgoing, PLANE)
    labels = jnp.arange(block_owner.shape[0], dtype=jnp.int32)
    code = block_owner * CAP + block_slot
    hits = block_ids[:, None] == labels[None, :]
    code_here = jnp.sum(jnp.where(hits, code[None, :], 0), axis=1)
    dest = code_here // CAP
    first = pack(snap_late, dest, members, 0, block, SUM_ROWS)
    arrived = exchange(mix(partial, code_here[None, :], first))
    modes, operator = settle(arrived, row_total, block)
    return (modes, operator)


def solution(mesh):
    split = jax.sharding.Mesh(mesh.devices.reshape((4, 4, 4, 2)), AXES)
    placed = (
        P(AXES, None, None),
        P(AXES, None, None),
        P(AXES),
        P(),
        P(),
    )
    return jax.shard_map(
        body,
        mesh=split,
        in_specs=placed,
        out_specs=(P(AXES, None, None), P()),
        check_vma=False,
    )
```

```python
import functools

import jax
import jax.numpy as jnp
from jax import lax
from jax.experimental import pallas as pl
from jax.experimental.pallas import tpu as pltpu
from jax.sharding import PartitionSpec as P

AXES = ("y", "x", "z", "core")
PLANE = ("x", "z", "core")
GRAM_CHUNKS = (16, 32, 48)
APPLY_STEP = 16
SUM_ROWS = 8
PIVOTS = 4
SHRINK = 32
CAP = 128


def split_pair(x):
    hi = x.astype(jnp.bfloat16)
    lo = (x - hi.astype(jnp.float32)).astype(jnp.bfloat16)
    return hi, lo


def contract_rows(a, b):
    return lax.dot_general(
        a, b, (((0,), (0,)), ((), ())), preferred_element_type=jnp.float32
    )


def gram_kernel(
    early_ref,
    late_ref,
    ids_ref,
    owner_ref,
    slot_ref,
    out_ref,
    first_ref,
    code_ref,
    early_buf,
    late_buf,
    ids_buf,
    owner_buf,
    slot_buf,
    code_buf,
    code_now,
    sem_early,
    sem_late,
    sem_table,
    sem_code,
    sem_out,
):
    count, block, width = late_ref.shape
    tables = []
    for k, (source, target) in enumerate(
        ((ids_ref, ids_buf), (owner_ref, owner_buf), (slot_ref, slot_buf))
    ):
        tables.append(pltpu.make_async_copy(source, target, sem_table.at[k]))
        tables[-1].start()
    parts = []
    lo = 0
    for k, size in enumerate(GRAM_CHUNKS):
        part = pl.ds(lo, size)
        one = pltpu.make_async_copy(early_ref.at[part], early_buf.at[part], sem_early.at[k])
        two = pltpu.make_async_copy(late_ref.at[part], late_buf.at[part], sem_late.at[k])
        one.start()
        two.start()
        parts.append((lo, size, one, two))
        lo += size

    for copy in tables:
        copy.wait()
    ids = ids_buf[...]
    lines, lanes = owner_buf.shape
    line_id = lax.broadcasted_iota(jnp.int32, (lines, count), 0)
    lane_id = lax.broadcasted_iota(jnp.int32, (lanes, count), 0)
    line = (line_id == jnp.right_shift(ids, 7)).astype(jnp.float32).astype(jnp.bfloat16)
    table = jnp.concatenate([owner_buf[...], slot_buf[...]], axis=1)
    found = contract_rows(table.astype(jnp.float32).astype(jnp.bfloat16), line)
    here = lane_id == jnp.bitwise_and(ids, lanes - 1)
    owner = jnp.sum(jnp.where(here, found[0:lanes], 0.0), axis=0, keepdims=True)
    slot = jnp.sum(jnp.where(here, found[lanes:], 0.0), axis=0, keepdims=True)
    code = (owner * CAP + slot).astype(jnp.int32)
    code_ref[...] = code
    code_buf[...] = jnp.zeros_like(code_buf)
    code_buf[:, 0:count] = code
    code_copy = pltpu.make_async_copy(code_buf, code_now, sem_code)
    code_copy.start()

    gram_wide = cross_wide = None
    for k, (lo, size, one, two) in enumerate(parts):
        two.wait()
        if k == 0:
            code_copy.wait()

        def send(i, carry):
            peer = jnp.right_shift(code_now[0, i], 7)
            pltpu.make_async_copy(
                late_buf.at[i], first_ref.at[peer, pl.ds(0, block)], sem_out
            ).start()
            return carry

        lax.fori_loop(lo, lo + size, send, 0, unroll=8)
        one.wait()
        part = pl.ds(lo, size)
        ehi, elo = split_pair(early_buf[part].reshape((-1, width)))
        lhi, llo = split_pair(late_buf[part].reshape((-1, width)))
        pair = jnp.concatenate([ehi, elo], axis=1)
        gram_part = contract_rows(ehi, pair)
        cross_part = contract_rows(pair, jnp.concatenate([lhi, llo], axis=1))
        gram_wide = gram_part if gram_wide is None else gram_wide + gram_part
        cross_wide = cross_part if cross_wide is None else cross_wide + cross_part
    mixed = gram_wide[:, width:]
    gram = gram_wide[:, 0:width] + (mixed + mixed.T)
    cross = cross_wide[0:width, 0:width] + (
        cross_wide[0:width, width:] + cross_wide[width:, 0:width]
    )
    size = out_ref.shape[0]
    half = SUM_ROWS // 2
    for r in range(half):
        out_ref[:, r, :] = gram[r * size : (r + 1) * size, :]
        out_ref[:, half + r, :] = cross[r * size : (r + 1) * size, :]
    pltpu.make_async_copy(
        late_buf, first_ref.at[pl.ds(0, count), pl.ds(0, block)], sem_out
    ).wait()


def gram_and_pack(early, late, ids, owner, slot, members):
    count, block, width = late.shape
    steps = len(GRAM_CHUNKS)
    anywhere = pl.BlockSpec(memory_space=pl.ANY)
    whole = pl.BlockSpec(memory_space=pltpu.VMEM)
    return pl.pallas_call(
        gram_kernel,
        in_specs=[anywhere] * 5,
        out_specs=(whole, anywhere, whole),
        out_shape=(
            jax.ShapeDtypeStruct((2 * width // SUM_ROWS, SUM_ROWS, width), jnp.float32),
            jax.ShapeDtypeStruct((members, block + SUM_ROWS, width), jnp.float32),
            jax.ShapeDtypeStruct((1, count), jnp.int32),
        ),
        scratch_shapes=[
            pltpu.VMEM((count, block, width), jnp.float32),
            pltpu.VMEM((count, block, width), jnp.float32),
            pltpu.VMEM(ids.shape, jnp.int32),
            pltpu.VMEM(owner.shape, jnp.int32),
            pltpu.VMEM(slot.shape, jnp.int32),
            pltpu.VMEM((1, CAP), jnp.int32),
            pltpu.SMEM((1, CAP), jnp.int32),
            pltpu.SemaphoreType.DMA((steps,)),
            pltpu.SemaphoreType.DMA((steps,)),
            pltpu.SemaphoreType.DMA((3,)),
            pltpu.SemaphoreType.DMA,
            pltpu.SemaphoreType.DMA,
        ],
        cost_estimate=pl.CostEstimate(
            flops=12 * count * block * width * width, bytes_accessed=1 << 23, transcendentals=0
        ),
        name="gram",
    )(early, late, ids, owner, slot)


def mix_kernel(partial_ref, code_ref, first_ref, out_ref, rows, sem):
    members, _, width = rows.shape
    total = jnp.sum(partial_ref[...], axis=0, keepdims=True)
    rows[...] = jnp.broadcast_to(total, rows.shape)
    mark = SUM_ROWS // 2 - 1
    code = code_ref[...]
    peer = lax.broadcasted_iota(jnp.int32, (members, code.shape[1]), 0)
    slot = (jnp.bitwise_and(code, CAP - 1) + 1).astype(jnp.float32)
    here = jnp.where(jnp.right_shift(code, 7) == peer, slot, 0.0)
    note = jnp.sum(here, axis=1, keepdims=True)
    lane = lax.broadcasted_iota(jnp.int32, (members, width), 1)
    rows[:, mark, :] = jnp.where(lane == 0, note, total[0, mark : mark + 1, :])
    tail = pl.ds(out_ref.shape[1] - SUM_ROWS, SUM_ROWS)
    copy = pltpu.make_async_copy(rows, out_ref.at[:, tail], sem)
    copy.start()
    copy.wait()


def mix(partial, code, first):
    members, _, width = first.shape
    whole = pl.BlockSpec(memory_space=pltpu.VMEM)
    anywhere = pl.BlockSpec(memory_space=pl.ANY)
    return pl.pallas_call(
        mix_kernel,
        in_specs=[whole, whole, anywhere],
        out_specs=anywhere,
        out_shape=jax.ShapeDtypeStruct(first.shape, first.dtype),
        scratch_shapes=[
            pltpu.VMEM((members, SUM_ROWS, width), jnp.float32),
            pltpu.SemaphoreType.DMA,
        ],
        input_output_aliases={2: 0},
        cost_estimate=pl.CostEstimate(flops=1000000, bytes_accessed=1 << 19, transcendentals=0),
        compiler_params=pltpu.CompilerParams(vmem_limit_bytes=57 << 20),
        name="mix",
    )(partial, code, first)


def dot3(a, b):
    return jnp.dot(a, b, precision=lax.Precision.HIGHEST, preferred_element_type=jnp.float32)


def eliminate(work, beside):
    order = work.shape[0]
    lane = lax.broadcasted_iota(jnp.int32, (1, 2 * order), 1)
    lane_half = lax.broadcasted_iota(jnp.int32, (1, order), 1)

    def step(lo, k, carry):
        j = lo + k * PIVOTS
        beside(lo // PIVOTS + k)
        row_id = lo + lax.broadcasted_iota(jnp.int32, (order - lo, 1), 0)
        table = work[lo:order, :]
        left = table[:, 0:order]
        rows = []
        columns = []
        for p in range(PIVOTS):
            rows.append(work[pl.ds(j + p, 1), :])
            picked = jnp.where(lane_half == j + p, left, 0.0)
            columns.append(jnp.sum(picked, axis=1, keepdims=True))
        block = {}
        for p in range(PIVOTS):
            for q in range(p, PIVOTS):
                picked = jnp.where(lane == j + q, rows[p], 0.0)
                block[p, q] = jnp.sum(picked, axis=1, keepdims=True)
        upper = {}
        for p in range(PIVOTS):
            pivot = block[p, p]
            for m in range(p):
                pivot = pivot - upper[m, p] * upper[m, p]
            inv = lax.rsqrt(pivot)
            for q in range(p + 1, PIVOTS):
                entry = block[p, q]
                for m in range(p):
                    entry = entry - upper[m, p] * upper[m, q]
                upper[p, q] = entry * inv
            for m in range(p):
                rows[p] = rows[p] - upper[m, p] * rows[m]
                columns[p] = columns[p] - upper[m, p] * columns[m]
            rows[p] = rows[p] * inv
            columns[p] = columns[p] * inv
        below = row_id >= j + PIVOTS
        for p in range(PIVOTS):
            table = table - jnp.where(below, columns[p], 0.0) * rows[p]
        for p in range(PIVOTS):
            table = jnp.where(row_id == j + p, rows[p], table)
        work[lo:order, :] = table
        return carry

    for lo in range(0, order, SHRINK):
        lax.fori_loop(0, SHRINK // PIVOTS, functools.partial(step, lo), 0)


def settle_kernel(
    row_total,
    arrived_ref,
    modes_ref,
    operator_ref,
    buf_in,
    pairs,
    buf_out,
    stats_ref,
    work,
    weight_ref,
    place_ref,
    slots_ref,
    sem_stats,
    sem_in,
    sem_out,
    sem_place,
):
    count, block, width = modes_ref.shape
    order = width
    steps = count // APPLY_STEP
    stats_copy = pltpu.make_async_copy(
        arrived_ref.at[:, pl.ds(block, SUM_ROWS)], stats_ref, sem_stats
    )
    stats_copy.start()

    group = count * PIVOTS // order

    def fetch(k):
        part = pl.ds(k * group, group)
        return pltpu.make_async_copy(
            arrived_ref.at[part, pl.ds(0, block)], buf_in.at[part], sem_in.at[k]
        )

    def divide(k):
        fetch(k).wait()
        rows = buf_in[pl.ds(k * group, group)].reshape((group * block, width))
        pairs[k] = jnp.concatenate(split_pair(rows), axis=1)

    for k in range(count // group):
        fetch(k).start()
    stats_copy.wait()

    row_id = lax.broadcasted_iota(jnp.int32, (order, 1), 0)
    lane = lax.broadcasted_iota(jnp.int32, (1, order), 1)
    size = 2 * order // SUM_ROWS
    half = SUM_ROWS // 2
    total = stats_ref[0:size]
    for p in range(1, order // size):
        total = total + stats_ref[p * size : (p + 1) * size]
    gram = jnp.concatenate([total[:, r, :] for r in range(half)], axis=0)
    work[:, 0:order] = jnp.where(row_id > lane, gram.T, gram) / row_total
    work[:, order:] = (row_id == lane).astype(jnp.float32)

    note = jnp.broadcast_to(stats_ref[:, half - 1, 0:1], (count, count))
    empty = note == 0.0
    counted = empty.astype(jnp.bfloat16)
    below = (row_id > lane).astype(jnp.bfloat16)
    earlier = jnp.dot(below, counted, preferred_element_type=jnp.float32)
    filled = count - jnp.sum(counted.astype(jnp.float32), axis=0, keepdims=True)
    code = jnp.where(empty, filled + earlier + CAP, note - 1.0)
    place_ref[...] = code.T[0:1, :].astype(jnp.int32)
    place_copy = pltpu.make_async_copy(place_ref, slots_ref, sem_place)
    place_copy.start()

    eliminate(work, divide)
    inverse_t = work[:, order:]
    inverse = inverse_t.T
    whi, wlo = split_pair(inverse)
    weight_ref[0:order, 0:order] = whi
    weight_ref[0:order, order:] = wlo
    weight_ref[order:, 0:order] = whi
    weight_ref[order:, order:] = wlo
    place_copy.wait()

    def step(t, carry):
        part = pl.ds(t * APPLY_STEP, APPLY_STEP)
        groups = APPLY_STEP // group
        rows = pairs[pl.ds(t * groups, groups)].reshape((APPLY_STEP * block, 2 * width))
        wide = jnp.dot(rows, weight_ref[...], preferred_element_type=jnp.float32)
        solved = wide[:, 0:width] + wide[:, width:]
        buf_out[part] = solved.reshape((APPLY_STEP, block, width))
        for i in range(APPLY_STEP):
            row = t * APPLY_STEP + i
            slot = slots_ref[0, row]

            @pl.when(slot >= CAP)
            def _():
                buf_out[row] = jnp.zeros((block, width), jnp.float32)

            pltpu.make_async_copy(
                buf_out.at[row], modes_ref.at[jnp.bitwise_and(slot, CAP - 1)], sem_out
            ).start()
        return carry

    lax.fori_loop(0, steps, step, 0)
    cross = jnp.concatenate([total[:, half + r, :] for r in range(half)], axis=0) / row_total
    operator_ref[...] = dot3(inverse_t, dot3(cross, inverse))
    pltpu.make_async_copy(buf_out, modes_ref, sem_out).wait()


def settle(arrived, row_total, block):
    count, _, width = arrived.shape
    anywhere = pl.BlockSpec(memory_space=pl.ANY)
    rows = pltpu.VMEM((count, block, width), jnp.float32)
    groups = width // PIVOTS
    return pl.pallas_call(
        functools.partial(settle_kernel, float(row_total)),
        in_specs=[anywhere],
        out_specs=(anywhere, pl.BlockSpec(memory_space=pltpu.VMEM)),
        out_shape=(
            jax.ShapeDtypeStruct((count, block, width), jnp.float32),
            jax.ShapeDtypeStruct((width, width), jnp.float32),
        ),
        scratch_shapes=[
            rows,
            pltpu.VMEM((groups, count * block // groups, 2 * width), jnp.bfloat16),
            rows,
            pltpu.VMEM((count, SUM_ROWS, width), jnp.float32),
            pltpu.VMEM((width, 2 * width), jnp.float32),
            pltpu.VMEM((2 * width, 2 * width), jnp.bfloat16),
            pltpu.VMEM((1, count), jnp.int32),
            pltpu.SMEM((1, count), jnp.int32),
            pltpu.SemaphoreType.DMA,
            pltpu.SemaphoreType.DMA((groups,)),
            pltpu.SemaphoreType.DMA,
            pltpu.SemaphoreType.DMA,
        ],
        cost_estimate=pl.CostEstimate(
            flops=8 * count * block * width * width, bytes_accessed=1 << 23, transcendentals=0
        ),
        name="settle",
    )(arrived)


def exchange(payload, axes=AXES):
    return lax.all_to_all(payload, axes, split_axis=0, concat_axis=0, tiled=True)


def body(snap_early, snap_late, block_ids, block_owner, block_slot):
    members = lax.axis_size(AXES)
    count, block, _ = snap_late.shape
    row_total = count * block * members
    outgoing, first, code = gram_and_pack(
        snap_early,
        snap_late,
        block_ids.reshape((1, count)),
        block_owner.reshape((-1, CAP)),
        block_slot.reshape((-1, CAP)),
        members,
    )
    partial = exchange(outgoing, PLANE)
    arrived = exchange(mix(partial, code, first))
    modes, operator = settle(arrived, row_total, block)
    return (modes, operator)


def solution(mesh):
    split = jax.sharding.Mesh(mesh.devices.reshape((4, 4, 4, 2)), AXES)
    placed = (
        P(AXES, None, None),
        P(AXES, None, None),
        P(AXES),
        P(),
        P(),
    )
    return jax.shard_map(
        body,
        mesh=split,
        in_specs=placed,
        out_specs=(P(AXES, None, None), P()),
        check_vma=False,
    )
```

```python
import functools

import jax
import jax.numpy as jnp
from jax import lax
from jax.experimental import pallas as pl
from jax.experimental.pallas import tpu as pltpu
from jax.sharding import PartitionSpec as P

AXES = ("y", "x", "z", "core")
PLANE = ("x", "z", "core")
GRAM_CHUNKS = (16, 32, 48)
APPLY_STEP = 64
SUM_ROWS = 8
PIVOTS = 4
SHRINK = 16
CAP = 128


def split_pair(x):
    hi = x.astype(jnp.bfloat16)
    lo = (x - hi.astype(jnp.float32)).astype(jnp.bfloat16)
    return hi, lo


def contract_rows(a, b):
    return lax.dot_general(
        a, b, (((0,), (0,)), ((), ())), preferred_element_type=jnp.float32
    )


def gram_kernel(
    early_ref,
    late_ref,
    ids_ref,
    owner_ref,
    slot_ref,
    out_ref,
    first_ref,
    code_ref,
    early_buf,
    late_buf,
    ids_buf,
    owner_buf,
    slot_buf,
    code_buf,
    code_now,
    sem_early,
    sem_late,
    sem_table,
    sem_code,
    sem_out,
):
    count, block, width = late_ref.shape
    tables = []
    for k, (source, target) in enumerate(
        ((ids_ref, ids_buf), (owner_ref, owner_buf), (slot_ref, slot_buf))
    ):
        tables.append(pltpu.make_async_copy(source, target, sem_table.at[k]))
        tables[-1].start()
    parts = []
    lo = 0
    for k, size in enumerate(GRAM_CHUNKS):
        part = pl.ds(lo, size)
        one = pltpu.make_async_copy(early_ref.at[part], early_buf.at[part], sem_early.at[k])
        two = pltpu.make_async_copy(late_ref.at[part], late_buf.at[part], sem_late.at[k])
        one.start()
        two.start()
        parts.append((lo, size, one, two))
        lo += size

    for copy in tables:
        copy.wait()
    ids = ids_buf[...]
    lines, lanes = owner_buf.shape
    line_id = lax.broadcasted_iota(jnp.int32, (lines, count), 0)
    lane_id = lax.broadcasted_iota(jnp.int32, (lanes, count), 0)
    line = (line_id == jnp.right_shift(ids, 7)).astype(jnp.float32).astype(jnp.bfloat16)
    table = jnp.concatenate([owner_buf[...], slot_buf[...]], axis=1)
    found = contract_rows(table.astype(jnp.float32).astype(jnp.bfloat16), line)
    here = lane_id == jnp.bitwise_and(ids, lanes - 1)
    owner = jnp.sum(jnp.where(here, found[0:lanes], 0.0), axis=0, keepdims=True)
    slot = jnp.sum(jnp.where(here, found[lanes:], 0.0), axis=0, keepdims=True)
    code = (owner * CAP + slot).astype(jnp.int32)
    code_ref[...] = code
    code_buf[...] = jnp.zeros_like(code_buf)
    code_buf[:, 0:count] = code
    code_copy = pltpu.make_async_copy(code_buf, code_now, sem_code)
    code_copy.start()

    gram_wide = cross_wide = None
    for k, (lo, size, one, two) in enumerate(parts):
        two.wait()
        if k == 0:
            code_copy.wait()

        def send(i, carry):
            peer = jnp.right_shift(code_now[0, i], 7)
            pltpu.make_async_copy(
                late_buf.at[i], first_ref.at[peer, pl.ds(0, block)], sem_out
            ).start()
            return carry

        lax.fori_loop(lo, lo + size, send, 0, unroll=8)
        one.wait()
        part = pl.ds(lo, size)
        ehi, elo = split_pair(early_buf[part].reshape((-1, width)))
        lhi, llo = split_pair(late_buf[part].reshape((-1, width)))
        pair = jnp.concatenate([ehi, elo], axis=1)
        gram_part = contract_rows(ehi, pair)
        cross_part = contract_rows(pair, jnp.concatenate([lhi, llo], axis=1))
        gram_wide = gram_part if gram_wide is None else gram_wide + gram_part
        cross_wide = cross_part if cross_wide is None else cross_wide + cross_part
    mixed = gram_wide[:, width:]
    gram = gram_wide[:, 0:width] + (mixed + mixed.T)
    cross = cross_wide[0:width, 0:width] + (
        cross_wide[0:width, width:] + cross_wide[width:, 0:width]
    )
    size = out_ref.shape[0]
    half = SUM_ROWS // 2
    for r in range(half):
        out_ref[:, r, :] = gram[r * size : (r + 1) * size, :]
        out_ref[:, half + r, :] = cross[r * size : (r + 1) * size, :]
    pltpu.make_async_copy(
        late_buf, first_ref.at[pl.ds(0, count), pl.ds(0, block)], sem_out
    ).wait()


def gram_and_pack(early, late, ids, owner, slot, members):
    count, block, width = late.shape
    steps = len(GRAM_CHUNKS)
    anywhere = pl.BlockSpec(memory_space=pl.ANY)
    whole = pl.BlockSpec(memory_space=pltpu.VMEM)
    return pl.pallas_call(
        gram_kernel,
        in_specs=[anywhere] * 5,
        out_specs=(whole, anywhere, whole),
        out_shape=(
            jax.ShapeDtypeStruct((2 * width // SUM_ROWS, SUM_ROWS, width), jnp.float32),
            jax.ShapeDtypeStruct((members, block + SUM_ROWS, width), jnp.float32),
            jax.ShapeDtypeStruct((1, count), jnp.int32),
        ),
        scratch_shapes=[
            pltpu.VMEM((count, block, width), jnp.float32),
            pltpu.VMEM((count, block, width), jnp.float32),
            pltpu.VMEM(ids.shape, jnp.int32),
            pltpu.VMEM(owner.shape, jnp.int32),
            pltpu.VMEM(slot.shape, jnp.int32),
            pltpu.VMEM((1, CAP), jnp.int32),
            pltpu.SMEM((1, CAP), jnp.int32),
            pltpu.SemaphoreType.DMA((steps,)),
            pltpu.SemaphoreType.DMA((steps,)),
            pltpu.SemaphoreType.DMA((3,)),
            pltpu.SemaphoreType.DMA,
            pltpu.SemaphoreType.DMA,
        ],
        cost_estimate=pl.CostEstimate(
            flops=12 * count * block * width * width, bytes_accessed=1 << 23, transcendentals=0
        ),
        name="gram",
    )(early, late, ids, owner, slot)


def mix_kernel(partial_ref, code_ref, first_ref, out_ref, rows, sem):
    members, _, width = rows.shape
    total = jnp.sum(partial_ref[...], axis=0, keepdims=True)
    rows[...] = jnp.broadcast_to(total, rows.shape)
    mark = SUM_ROWS // 2 - 1
    code = code_ref[...]
    peer = lax.broadcasted_iota(jnp.int32, (members, code.shape[1]), 0)
    slot = (jnp.bitwise_and(code, CAP - 1) + 1).astype(jnp.float32)
    here = jnp.where(jnp.right_shift(code, 7) == peer, slot, 0.0)
    note = jnp.sum(here, axis=1, keepdims=True)
    lane = lax.broadcasted_iota(jnp.int32, (members, width), 1)
    rows[:, mark, :] = jnp.where(lane == 0, note, total[0, mark : mark + 1, :])
    tail = pl.ds(out_ref.shape[1] - SUM_ROWS, SUM_ROWS)
    copy = pltpu.make_async_copy(rows, out_ref.at[:, tail], sem)
    copy.start()
    copy.wait()


def mix(partial, code, first):
    members, _, width = first.shape
    whole = pl.BlockSpec(memory_space=pltpu.VMEM)
    anywhere = pl.BlockSpec(memory_space=pl.ANY)
    return pl.pallas_call(
        mix_kernel,
        in_specs=[whole, whole, anywhere],
        out_specs=anywhere,
        out_shape=jax.ShapeDtypeStruct(first.shape, first.dtype),
        scratch_shapes=[
            pltpu.VMEM((members, SUM_ROWS, width), jnp.float32),
            pltpu.SemaphoreType.DMA,
        ],
        input_output_aliases={2: 0},
        cost_estimate=pl.CostEstimate(flops=1000000, bytes_accessed=1 << 19, transcendentals=0),
        compiler_params=pltpu.CompilerParams(vmem_limit_bytes=57 << 20),
        name="mix",
    )(partial, code, first)


def dot3(a, b):
    return jnp.dot(a, b, precision=lax.Precision.HIGHEST, preferred_element_type=jnp.float32)


def eliminate(work):
    order = work.shape[0]
    lane = lax.broadcasted_iota(jnp.int32, (1, 2 * order), 1)
    lane_half = lax.broadcasted_iota(jnp.int32, (1, order), 1)

    def step(lo, k, carry):
        j = lo + k * PIVOTS
        row_id = lo + lax.broadcasted_iota(jnp.int32, (order - lo, 1), 0)
        table = work[lo:order, :]
        left = table[:, 0:order]
        rows = []
        columns = []
        for p in range(PIVOTS):
            rows.append(work[pl.ds(j + p, 1), :])
            picked = jnp.where(lane_half == j + p, left, 0.0)
            columns.append(jnp.sum(picked, axis=1, keepdims=True))
        block = {}
        for p in range(PIVOTS):
            for q in range(p, PIVOTS):
                picked = jnp.where(lane == j + q, rows[p], 0.0)
                block[p, q] = jnp.sum(picked, axis=1, keepdims=True)
        upper = {}
        for p in range(PIVOTS):
            pivot = block[p, p]
            for m in range(p):
                pivot = pivot - upper[m, p] * upper[m, p]
            inv = lax.rsqrt(pivot)
            for q in range(p + 1, PIVOTS):
                entry = block[p, q]
                for m in range(p):
                    entry = entry - upper[m, p] * upper[m, q]
                upper[p, q] = entry * inv
            for m in range(p):
                rows[p] = rows[p] - upper[m, p] * rows[m]
                columns[p] = columns[p] - upper[m, p] * columns[m]
            rows[p] = rows[p] * inv
            columns[p] = columns[p] * inv
        below = row_id >= j + PIVOTS
        for p in range(PIVOTS):
            table = table - jnp.where(below, columns[p], 0.0) * rows[p]
        for p in range(PIVOTS):
            table = jnp.where(row_id == j + p, rows[p], table)
        work[lo:order, :] = table
        return carry

    for lo in range(0, order, SHRINK):
        lax.fori_loop(0, SHRINK // PIVOTS, functools.partial(step, lo), 0)


def settle_kernel(
    row_total,
    arrived_ref,
    modes_ref,
    operator_ref,
    buf_in,
    buf_out,
    stats_ref,
    work,
    weight_ref,
    place_ref,
    slots_ref,
    sem_stats,
    sem_in,
    sem_out,
    sem_place,
):
    count, block, width = modes_ref.shape
    order = width
    steps = count // APPLY_STEP
    stats_copy = pltpu.make_async_copy(
        arrived_ref.at[:, pl.ds(block, SUM_ROWS)], stats_ref, sem_stats
    )
    stats_copy.start()

    def fetch(t):
        part = pl.ds(t * APPLY_STEP, APPLY_STEP)
        return pltpu.make_async_copy(
            arrived_ref.at[part, pl.ds(0, block)], buf_in.at[part], sem_in.at[t]
        )

    for t in range(steps):
        fetch(t).start()
    stats_copy.wait()

    row_id = lax.broadcasted_iota(jnp.int32, (order, 1), 0)
    lane = lax.broadcasted_iota(jnp.int32, (1, order), 1)
    size = 2 * order // SUM_ROWS
    half = SUM_ROWS // 2
    total = stats_ref[0:size]
    for p in range(1, order // size):
        total = total + stats_ref[p * size : (p + 1) * size]
    gram = jnp.concatenate([total[:, r, :] for r in range(half)], axis=0)
    work[:, 0:order] = jnp.where(row_id > lane, gram.T, gram) / row_total
    work[:, order:] = (row_id == lane).astype(jnp.float32)

    note = jnp.broadcast_to(stats_ref[:, half - 1, 0:1], (count, count))
    empty = note == 0.0
    counted = empty.astype(jnp.bfloat16)
    below = (row_id > lane).astype(jnp.bfloat16)
    earlier = jnp.dot(below, counted, preferred_element_type=jnp.float32)
    filled = count - jnp.sum(counted.astype(jnp.float32), axis=0, keepdims=True)
    code = jnp.where(empty, filled + earlier + CAP, note - 1.0)
    place_ref[...] = code.T[0:1, :].astype(jnp.int32)
    place_copy = pltpu.make_async_copy(place_ref, slots_ref, sem_place)
    place_copy.start()

    eliminate(work)
    inverse_t = work[:, order:]
    inverse = inverse_t.T
    whi, wlo = split_pair(inverse)
    weight_ref[0:order, 0:order] = whi
    weight_ref[0:order, order:] = wlo
    weight_ref[order:, 0:order] = whi
    weight_ref[order:, order:] = wlo
    place_copy.wait()

    def step(t, carry):
        part = pl.ds(t * APPLY_STEP, APPLY_STEP)
        fetch(t).wait()
        hi, low = split_pair(buf_in[part].reshape((APPLY_STEP * block, width)))
        wide = jnp.dot(
            jnp.concatenate([hi, low], axis=1),
            weight_ref[...],
            preferred_element_type=jnp.float32,
        )
        solved = wide[:, 0:width] + wide[:, width:]
        buf_out[part] = solved.reshape((APPLY_STEP, block, width))
        for i in range(APPLY_STEP):
            row = t * APPLY_STEP + i
            slot = slots_ref[0, row]

            @pl.when(slot >= CAP)
            def _():
                buf_out[row] = jnp.zeros((block, width), jnp.float32)

            pltpu.make_async_copy(
                buf_out.at[row], modes_ref.at[jnp.bitwise_and(slot, CAP - 1)], sem_out
            ).start()
        return carry

    lax.fori_loop(0, steps, step, 0)
    cross = jnp.concatenate([total[:, half + r, :] for r in range(half)], axis=0) / row_total
    operator_ref[...] = dot3(inverse_t, dot3(cross, inverse))
    pltpu.make_async_copy(buf_out, modes_ref, sem_out).wait()


def settle(arrived, row_total, block):
    count, _, width = arrived.shape
    anywhere = pl.BlockSpec(memory_space=pl.ANY)
    rows = pltpu.VMEM((count, block, width), jnp.float32)
    return pl.pallas_call(
        functools.partial(settle_kernel, float(row_total)),
        in_specs=[anywhere],
        out_specs=(anywhere, pl.BlockSpec(memory_space=pltpu.VMEM)),
        out_shape=(
            jax.ShapeDtypeStruct((count, block, width), jnp.float32),
            jax.ShapeDtypeStruct((width, width), jnp.float32),
        ),
        scratch_shapes=[
            rows,
            rows,
            pltpu.VMEM((count, SUM_ROWS, width), jnp.float32),
            pltpu.VMEM((width, 2 * width), jnp.float32),
            pltpu.VMEM((2 * width, 2 * width), jnp.bfloat16),
            pltpu.VMEM((1, count), jnp.int32),
            pltpu.SMEM((1, count), jnp.int32),
            pltpu.SemaphoreType.DMA,
            pltpu.SemaphoreType.DMA((count // APPLY_STEP,)),
            pltpu.SemaphoreType.DMA,
            pltpu.SemaphoreType.DMA,
        ],
        cost_estimate=pl.CostEstimate(
            flops=8 * count * block * width * width, bytes_accessed=1 << 23, transcendentals=0
        ),
        name="settle",
    )(arrived)


def exchange(payload, axes=AXES):
    return lax.all_to_all(payload, axes, split_axis=0, concat_axis=0, tiled=True)


def body(snap_early, snap_late, block_ids, block_owner, block_slot):
    members = lax.axis_size(AXES)
    count, block, _ = snap_late.shape
    row_total = count * block * members
    outgoing, first, code = gram_and_pack(
        snap_early,
        snap_late,
        block_ids.reshape((1, count)),
        block_owner.reshape((-1, CAP)),
        block_slot.reshape((-1, CAP)),
        members,
    )
    partial = exchange(outgoing, PLANE)
    arrived = exchange(mix(partial, code, first))
    modes, operator = settle(arrived, row_total, block)
    return (modes, operator)


def solution(mesh):
    split = jax.sharding.Mesh(mesh.devices.reshape((4, 4, 4, 2)), AXES)
    placed = (
        P(AXES, None, None),
        P(AXES, None, None),
        P(AXES),
        P(),
        P(),
    )
    return jax.shard_map(
        body,
        mesh=split,
        in_specs=placed,
        out_specs=(P(AXES, None, None), P()),
        check_vma=False,
    )
```

```python
import functools

import jax
import jax.numpy as jnp
from jax import lax
from jax.experimental import pallas as pl
from jax.experimental.pallas import tpu as pltpu
from jax.sharding import PartitionSpec as P

AXES = ("y", "x", "z", "core")
PLANE = ("x", "z", "core")
GRAM_CHUNKS = (16, 32, 48)
APPLY_STEP = 64
SUM_ROWS = 8
PIVOTS = 4
SHRINK = 8
CAP = 128


def split_pair(x):
    hi = x.astype(jnp.bfloat16)
    lo = (x - hi.astype(jnp.float32)).astype(jnp.bfloat16)
    return hi, lo


def contract_rows(a, b):
    return lax.dot_general(
        a, b, (((0,), (0,)), ((), ())), preferred_element_type=jnp.float32
    )


def gram_kernel(
    early_ref,
    late_ref,
    ids_ref,
    owner_ref,
    slot_ref,
    out_ref,
    first_ref,
    code_ref,
    early_buf,
    late_buf,
    ids_buf,
    owner_buf,
    slot_buf,
    code_buf,
    code_now,
    sem_early,
    sem_late,
    sem_table,
    sem_code,
    sem_out,
):
    count, block, width = late_ref.shape
    tables = []
    for k, (source, target) in enumerate(
        ((ids_ref, ids_buf), (owner_ref, owner_buf), (slot_ref, slot_buf))
    ):
        tables.append(pltpu.make_async_copy(source, target, sem_table.at[k]))
        tables[-1].start()
    parts = []
    lo = 0
    for k, size in enumerate(GRAM_CHUNKS):
        part = pl.ds(lo, size)
        one = pltpu.make_async_copy(early_ref.at[part], early_buf.at[part], sem_early.at[k])
        two = pltpu.make_async_copy(late_ref.at[part], late_buf.at[part], sem_late.at[k])
        one.start()
        two.start()
        parts.append((lo, size, one, two))
        lo += size

    for copy in tables:
        copy.wait()
    ids = ids_buf[...]
    lines, lanes = owner_buf.shape
    line_id = lax.broadcasted_iota(jnp.int32, (lines, count), 0)
    lane_id = lax.broadcasted_iota(jnp.int32, (lanes, count), 0)
    line = (line_id == jnp.right_shift(ids, 7)).astype(jnp.float32).astype(jnp.bfloat16)
    table = jnp.concatenate([owner_buf[...], slot_buf[...]], axis=1)
    found = contract_rows(table.astype(jnp.float32).astype(jnp.bfloat16), line)
    here = lane_id == jnp.bitwise_and(ids, lanes - 1)
    owner = jnp.sum(jnp.where(here, found[0:lanes], 0.0), axis=0, keepdims=True)
    slot = jnp.sum(jnp.where(here, found[lanes:], 0.0), axis=0, keepdims=True)
    code = (owner * CAP + slot).astype(jnp.int32)
    code_ref[...] = code
    code_buf[...] = jnp.zeros_like(code_buf)
    code_buf[:, 0:count] = code
    code_copy = pltpu.make_async_copy(code_buf, code_now, sem_code)
    code_copy.start()

    gram_wide = cross_wide = None
    for k, (lo, size, one, two) in enumerate(parts):
        two.wait()
        if k == 0:
            code_copy.wait()

        def send(i, carry):
            peer = jnp.right_shift(code_now[0, i], 7)
            pltpu.make_async_copy(
                late_buf.at[i], first_ref.at[peer, pl.ds(0, block)], sem_out
            ).start()
            return carry

        lax.fori_loop(lo, lo + size, send, 0, unroll=8)
        one.wait()
        part = pl.ds(lo, size)
        ehi, elo = split_pair(early_buf[part].reshape((-1, width)))
        lhi, llo = split_pair(late_buf[part].reshape((-1, width)))
        pair = jnp.concatenate([ehi, elo], axis=1)
        gram_part = contract_rows(ehi, pair)
        cross_part = contract_rows(pair, jnp.concatenate([lhi, llo], axis=1))
        gram_wide = gram_part if gram_wide is None else gram_wide + gram_part
        cross_wide = cross_part if cross_wide is None else cross_wide + cross_part
    mixed = gram_wide[:, width:]
    gram = gram_wide[:, 0:width] + (mixed + mixed.T)
    cross = cross_wide[0:width, 0:width] + (
        cross_wide[0:width, width:] + cross_wide[width:, 0:width]
    )
    size = out_ref.shape[0]
    half = SUM_ROWS // 2
    for r in range(half):
        out_ref[:, r, :] = gram[r * size : (r + 1) * size, :]
        out_ref[:, half + r, :] = cross[r * size : (r + 1) * size, :]
    pltpu.make_async_copy(
        late_buf, first_ref.at[pl.ds(0, count), pl.ds(0, block)], sem_out
    ).wait()


def gram_and_pack(early, late, ids, owner, slot, members):
    count, block, width = late.shape
    steps = len(GRAM_CHUNKS)
    anywhere = pl.BlockSpec(memory_space=pl.ANY)
    whole = pl.BlockSpec(memory_space=pltpu.VMEM)
    return pl.pallas_call(
        gram_kernel,
        in_specs=[anywhere] * 5,
        out_specs=(whole, anywhere, whole),
        out_shape=(
            jax.ShapeDtypeStruct((2 * width // SUM_ROWS, SUM_ROWS, width), jnp.float32),
            jax.ShapeDtypeStruct((members, block + SUM_ROWS, width), jnp.float32),
            jax.ShapeDtypeStruct((1, count), jnp.int32),
        ),
        scratch_shapes=[
            pltpu.VMEM((count, block, width), jnp.float32),
            pltpu.VMEM((count, block, width), jnp.float32),
            pltpu.VMEM(ids.shape, jnp.int32),
            pltpu.VMEM(owner.shape, jnp.int32),
            pltpu.VMEM(slot.shape, jnp.int32),
            pltpu.VMEM((1, CAP), jnp.int32),
            pltpu.SMEM((1, CAP), jnp.int32),
            pltpu.SemaphoreType.DMA((steps,)),
            pltpu.SemaphoreType.DMA((steps,)),
            pltpu.SemaphoreType.DMA((3,)),
            pltpu.SemaphoreType.DMA,
            pltpu.SemaphoreType.DMA,
        ],
        cost_estimate=pl.CostEstimate(
            flops=12 * count * block * width * width, bytes_accessed=1 << 23, transcendentals=0
        ),
        name="gram",
    )(early, late, ids, owner, slot)


def mix_kernel(partial_ref, code_ref, first_ref, out_ref, rows, code_buf, sem, sem_code):
    members, _, width = rows.shape
    code_copy = pltpu.make_async_copy(code_ref, code_buf, sem_code)
    code_copy.start()
    total = jnp.sum(partial_ref[...], axis=0, keepdims=True)
    rows[...] = jnp.broadcast_to(total, rows.shape)
    mark = SUM_ROWS // 2 - 1
    code_copy.wait()
    code = code_buf[...]
    peer = lax.broadcasted_iota(jnp.int32, (members, code.shape[1]), 0)
    slot = (jnp.bitwise_and(code, CAP - 1) + 1).astype(jnp.float32)
    here = jnp.where(jnp.right_shift(code, 7) == peer, slot, 0.0)
    note = jnp.sum(here, axis=1, keepdims=True)
    lane = lax.broadcasted_iota(jnp.int32, (members, width), 1)
    rows[:, mark, :] = jnp.where(lane == 0, note, total[0, mark : mark + 1, :])
    tail = pl.ds(out_ref.shape[1] - SUM_ROWS, SUM_ROWS)
    copy = pltpu.make_async_copy(rows, out_ref.at[:, tail], sem)
    copy.start()
    copy.wait()


def mix(partial, code, first):
    members, _, width = first.shape
    whole = pl.BlockSpec(memory_space=pltpu.VMEM)
    anywhere = pl.BlockSpec(memory_space=pl.ANY)
    return pl.pallas_call(
        mix_kernel,
        in_specs=[whole, anywhere, anywhere],
        out_specs=anywhere,
        out_shape=jax.ShapeDtypeStruct(first.shape, first.dtype),
        scratch_shapes=[
            pltpu.VMEM((members, SUM_ROWS, width), jnp.float32),
            pltpu.VMEM(code.shape, jnp.int32),
            pltpu.SemaphoreType.DMA,
            pltpu.SemaphoreType.DMA,
        ],
        input_output_aliases={2: 0},
        cost_estimate=pl.CostEstimate(flops=1000000, bytes_accessed=1 << 19, transcendentals=0),
        compiler_params=pltpu.CompilerParams(vmem_limit_bytes=52 << 20),
        name="mix",
    )(partial, code, first)


def dot3(a, b):
    return jnp.dot(a, b, precision=lax.Precision.HIGHEST, preferred_element_type=jnp.float32)


def eliminate(work):
    order = work.shape[0]
    lane = lax.broadcasted_iota(jnp.int32, (1, 2 * order), 1)
    lane_half = lax.broadcasted_iota(jnp.int32, (1, order), 1)

    def step(lo, k, carry):
        j = lo + k * PIVOTS
        row_id = lo + lax.broadcasted_iota(jnp.int32, (order - lo, 1), 0)
        table = work[lo:order, :]
        left = table[:, 0:order]
        rows = []
        columns = []
        for p in range(PIVOTS):
            rows.append(work[pl.ds(j + p, 1), :])
            picked = jnp.where(lane_half == j + p, left, 0.0)
            columns.append(jnp.sum(picked, axis=1, keepdims=True))
        block = {}
        for p in range(PIVOTS):
            for q in range(p, PIVOTS):
                picked = jnp.where(lane == j + q, rows[p], 0.0)
                block[p, q] = jnp.sum(picked, axis=1, keepdims=True)
        upper = {}
        for p in range(PIVOTS):
            pivot = block[p, p]
            for m in range(p):
                pivot = pivot - upper[m, p] * upper[m, p]
            inv = lax.rsqrt(pivot)
            for q in range(p + 1, PIVOTS):
                entry = block[p, q]
                for m in range(p):
                    entry = entry - upper[m, p] * upper[m, q]
                upper[p, q] = entry * inv
            for m in range(p):
                rows[p] = rows[p] - upper[m, p] * rows[m]
                columns[p] = columns[p] - upper[m, p] * columns[m]
            rows[p] = rows[p] * inv
            columns[p] = columns[p] * inv
        below = row_id >= j + PIVOTS
        for p in range(PIVOTS):
            table = table - jnp.where(below, columns[p], 0.0) * rows[p]
        for p in range(PIVOTS):
            table = jnp.where(row_id == j + p, rows[p], table)
        work[lo:order, :] = table
        return carry

    for lo in range(0, order, SHRINK):
        lax.fori_loop(0, SHRINK // PIVOTS, functools.partial(step, lo), 0)


def settle_kernel(
    row_total,
    arrived_ref,
    modes_ref,
    operator_ref,
    buf_in,
    buf_out,
    stats_ref,
    work,
    weight_ref,
    place_ref,
    slots_ref,
    sem_stats,
    sem_in,
    sem_out,
    sem_place,
):
    count, block, width = modes_ref.shape
    order = width
    steps = count // APPLY_STEP
    stats_copy = pltpu.make_async_copy(
        arrived_ref.at[:, pl.ds(block, SUM_ROWS)], stats_ref, sem_stats
    )
    stats_copy.start()

    def fetch(t):
        part = pl.ds(t * APPLY_STEP, APPLY_STEP)
        return pltpu.make_async_copy(
            arrived_ref.at[part, pl.ds(0, block)], buf_in.at[part], sem_in.at[t]
        )

    for t in range(steps):
        fetch(t).start()
    buf_out[count] = jnp.zeros((block, width), jnp.float32)
    stats_copy.wait()

    row_id = lax.broadcasted_iota(jnp.int32, (order, 1), 0)
    lane = lax.broadcasted_iota(jnp.int32, (1, order), 1)
    size = 2 * order // SUM_ROWS
    half = SUM_ROWS // 2
    total = stats_ref[0:size]
    for p in range(1, order // size):
        total = total + stats_ref[p * size : (p + 1) * size]
    gram = jnp.concatenate([total[:, r, :] for r in range(half)], axis=0)
    work[:, 0:order] = jnp.where(row_id > lane, gram.T, gram) / row_total
    work[:, order:] = (row_id == lane).astype(jnp.float32)

    note = jnp.broadcast_to(stats_ref[:, half - 1, 0:1], (count, count))
    empty = note == 0.0
    counted = empty.astype(jnp.bfloat16)
    below = (row_id > lane).astype(jnp.bfloat16)
    earlier = jnp.dot(below, counted, preferred_element_type=jnp.float32)
    filled = count - jnp.sum(counted.astype(jnp.float32), axis=0, keepdims=True)
    code = jnp.where(empty, filled + earlier + CAP, note - 1.0)
    place_ref[...] = code.T[0:1, :].astype(jnp.int32)
    place_copy = pltpu.make_async_copy(place_ref, slots_ref, sem_place)
    place_copy.start()

    eliminate(work)
    inverse_t = work[:, order:]
    inverse = inverse_t.T
    whi, wlo = split_pair(inverse)
    weight_ref[0:order, 0:order] = whi
    weight_ref[0:order, order:] = wlo
    weight_ref[order:, 0:order] = whi
    weight_ref[order:, order:] = wlo
    place_copy.wait()

    def step(t, carry):
        part = pl.ds(t * APPLY_STEP, APPLY_STEP)
        fetch(t).wait()
        hi, low = split_pair(buf_in[part].reshape((APPLY_STEP * block, width)))
        wide = jnp.dot(
            jnp.concatenate([hi, low], axis=1),
            weight_ref[...],
            preferred_element_type=jnp.float32,
        )
        solved = wide[:, 0:width] + wide[:, width:]
        buf_out[part] = solved.reshape((APPLY_STEP, block, width))
        for i in range(APPLY_STEP):
            row = t * APPLY_STEP + i
            slot = slots_ref[0, row]
            source = jnp.where(slot >= CAP, count, row)
            pltpu.make_async_copy(
                buf_out.at[source], modes_ref.at[jnp.bitwise_and(slot, CAP - 1)], sem_out
            ).start()
        return carry

    lax.fori_loop(0, steps, step, 0)
    cross = jnp.concatenate([total[:, half + r, :] for r in range(half)], axis=0) / row_total
    operator_ref[...] = dot3(inverse_t, dot3(cross, inverse))
    pltpu.make_async_copy(buf_out.at[pl.ds(0, count)], modes_ref, sem_out).wait()


def settle(arrived, row_total, block):
    count, _, width = arrived.shape
    anywhere = pl.BlockSpec(memory_space=pl.ANY)
    rows = pltpu.VMEM((count, block, width), jnp.float32)
    return pl.pallas_call(
        functools.partial(settle_kernel, float(row_total)),
        in_specs=[anywhere],
        out_specs=(anywhere, pl.BlockSpec(memory_space=pltpu.VMEM)),
        out_shape=(
            jax.ShapeDtypeStruct((count, block, width), jnp.float32),
            jax.ShapeDtypeStruct((width, width), jnp.float32),
        ),
        scratch_shapes=[
            rows,
            pltpu.VMEM((count + 1, block, width), jnp.float32),
            pltpu.VMEM((count, SUM_ROWS, width), jnp.float32),
            pltpu.VMEM((width, 2 * width), jnp.float32),
            pltpu.VMEM((2 * width, 2 * width), jnp.bfloat16),
            pltpu.VMEM((1, count), jnp.int32),
            pltpu.SMEM((1, count), jnp.int32),
            pltpu.SemaphoreType.DMA,
            pltpu.SemaphoreType.DMA((count // APPLY_STEP,)),
            pltpu.SemaphoreType.DMA,
            pltpu.SemaphoreType.DMA,
        ],
        cost_estimate=pl.CostEstimate(
            flops=8 * count * block * width * width, bytes_accessed=1 << 23, transcendentals=0
        ),
        name="settle",
    )(arrived)


def exchange(payload, axes=AXES):
    return lax.all_to_all(payload, axes, split_axis=0, concat_axis=0, tiled=True)


def body(snap_early, snap_late, block_ids, block_owner, block_slot):
    members = lax.axis_size(AXES)
    count, block, _ = snap_late.shape
    row_total = count * block * members
    outgoing, first, code = gram_and_pack(
        snap_early,
        snap_late,
        block_ids.reshape((1, count)),
        block_owner.reshape((-1, CAP)),
        block_slot.reshape((-1, CAP)),
        members,
    )
    partial = exchange(outgoing, PLANE)
    arrived = exchange(mix(partial, code, first))
    modes, operator = settle(arrived, row_total, block)
    return (modes, operator)


def solution(mesh):
    split = jax.sharding.Mesh(mesh.devices.reshape((4, 4, 4, 2)), AXES)
    placed = (
        P(AXES, None, None),
        P(AXES, None, None),
        P(AXES),
        P(),
        P(),
    )
    return jax.shard_map(
        body,
        mesh=split,
        in_specs=placed,
        out_specs=(P(AXES, None, None), P()),
        check_vma=False,
    )
```
